256 devices in a mesh: gx: 4 (over x), gy: 8 (over y, core), gz: 8 (over z).
Axes of the slice: x: 4, y: 4, z: 8, core: 2. Of those that a mesh axis runs over, the one named last changes fastest.
Arguments:
- ham_blocks: bfloat16 [2048, 128, 128], P(('gx', 'gy', 'gz')), may hold values from -0.119628906 to 0.119628906
- onsite: float32 [256, 768], P(('gx', 'gy', 'gz')), may hold values from -1 to 1
- entry_slot: int32 [256, 36], P(('gx', 'gy', 'gz')), may hold values from 0 to 63, as said below
- send_table: int32 [256, 64, 1], P(('gx', 'gy', 'gz')), may hold values from -1 to 7, as said below
- reads: int32 [256, 8], P(('gx', 'gy', 'gz')), may hold values from 0 to 42, as said below
- gram_targets: int32 [256, 7, 8], P(('gx', 'gy', 'gz')), may hold values from 0 to 36, as said below
- table_pick: int32 [256, 2, 8], P(('gx', 'gy', 'gz')), may hold values from 0 to 3, as said below
- phi: bfloat16 [256, 4, 128, 4096], P(('gx', 'gy', 'gz')), may hold values from -2.390625 to 2.390625
- potential_in: float32 [16, 64, 1024], P('gx', 'gy', 'gz'), may hold values from -1.5 to 1.5
Outputs:
- potential: float32 [16, 64, 1024], P('gx', 'gy', 'gz')
- grid_blocks: float32 [2048, 128, 128], P(('gx', 'gy', 'gz'))
The draws below stay inside these ranges and needn't reach their ends.
Inputs may be any that keep to these rules, and one draw needn't show every extreme that they name: `entry_slot`: row d holds distinct slot numbers; at most 1 entries of one submatrix come from one device of its plane, and some device gives exactly 1. send_table[o, e, c] is the local block that submatrix e of o's plane reads in slot o's plane number + c, and -1 where e reads no block in that slot. `reads`: 42 marks an unused slot; some brick uses all 8 slots; the number of used slots differs widely between bricks. gram_targets[d, k, r] is 36 where slot r of the brick at face k of d is unused, and an entry below 36 where it is used; one entry of a submatrix receives at most two slots. `table_pick`: the two tables of one slot differ.
All inputs are finite; a program needn't handle non-finite values.
Results may differ from the reference program's by a relative error of at most 0.012.
Values may be sent and summed in bfloat16 or wider, within the bound.
No kernel may reach another device: no remote copies, remote signals or barrier semaphores. Data moves between devices by JAX's collectives and lax.ppermute only.
A program may use at most 128 MiB of HBM per device.

```python
import jax
import jax.numpy as jnp
from jax import lax

B = 128
S = 6
M = 768
HB_DEV = 8
CAP = 1
RMAX = 8
NOV = 4
BX = 4
BY = 8
BZ = 128
G = 4096
NX = 16
NY = 64
NZ = 1024
HBLOCKS = 2048
N_GX = 4
N_GY = 8
N_GZ = 8
DEVICES = 256


SHIFTS_X = (0, -1, 1, 0, 0, 0, 0)


SHIFTS_Y = (0, 0, 0, -1, 1, 0, 0)


SHIFTS_Z = (0, 0, 0, 0, 0, -1, 1)


def neighbour_index(device, face):
    plane = N_GY * N_GZ
    coord_x = (device // plane + jnp.array(SHIFTS_X, jnp.int32)[face]) % N_GX
    coord_y = (device // N_GZ % N_GY + jnp.array(SHIFTS_Y, jnp.int32)[face]) % N_GY
    coord_z = (device % N_GZ + jnp.array(SHIFTS_Z, jnp.int32)[face]) % N_GZ
    return (coord_x * N_GY + coord_y) * N_GZ + coord_z


def request_tables(key):
    plane = N_GY * N_GZ
    count = N_GX * plane
    base = jax.random.fold_in(key, 7001)
    several = jax.random.split(base, count)
    orders = jax.vmap(lambda single: jax.random.permutation(single, plane * CAP))(several)
    positions = orders[:, :S * S].astype(jnp.int32)
    blocks = jax.random.randint(jax.random.fold_in(key, 7002), (count, S * S), 0, HB_DEV).astype(jnp.int32)
    devices = jnp.arange(count, dtype=jnp.int32)[:, None]
    owners = devices // plane * plane + positions // CAP
    targets = jnp.broadcast_to(devices % plane, positions.shape)
    lanes = positions % CAP
    table = jnp.full((count, plane, CAP), -1, jnp.int32).at[owners, targets, lanes].set(blocks)
    return (positions, table)


def reader_tables(key):
    count = DEVICES
    base = jax.random.fold_in(key, 8001)
    first = jax.random.randint(jax.random.fold_in(base, 1), (count,), 0, RMAX)
    used = 1 + first
    fullest = jax.random.randint(jax.random.fold_in(base, 3), (), 0, count)
    used = jnp.where(jnp.arange(count) == fullest, RMAX, used)
    codes = jax.random.randint(jax.random.fold_in(base, 4), (count, RMAX), 0, 7 * S).astype(jnp.int32)
    codes = jnp.where(jnp.arange(RMAX)[None, :] < used[:, None], codes, 7 * S).astype(jnp.int32)
    devices = jnp.arange(count, dtype=jnp.int32)[:, None]
    faces = jnp.arange(7, dtype=jnp.int32)[None, :]
    sources = neighbour_index(devices, faces)
    their = codes[sources]
    live = (their < 7 * S).reshape(count, 7 * RMAX).astype(jnp.int32)
    ranks = jnp.cumsum(live, axis=1) - live
    several = jax.random.split(jax.random.fold_in(base, 5), count)
    orders = jax.vmap(lambda single: jax.random.permutation(single, S * S))(several).astype(jnp.int32)
    entries = jnp.take_along_axis(orders, ranks % (S * S), axis=1)
    targets = jnp.where(live > 0, entries, S * S).astype(jnp.int32).reshape(count, 7, RMAX)
    return (codes, targets)


def draw_entry_slot(key, part):
    return request_tables(key)[0]


def draw_send_table(key, part):
    return request_tables(key)[1]


def draw_reads(key, part):
    return reader_tables(key)[0]


def draw_gram_targets(key, part):
    return reader_tables(key)[1]


def draw_table_pick(key, part):
    left = jax.random.randint(jax.random.fold_in(key, 9001), (DEVICES, RMAX), 0, NOV).astype(jnp.int32)
    step = jax.random.randint(jax.random.fold_in(key, 9002), (DEVICES, RMAX), 1, NOV).astype(jnp.int32)
    right = (left + step) % NOV
    return jnp.stack([left, right], axis=1).astype(jnp.int32)


def steps_of(stream_key, shape, shards, low, largest):
    def one(dim, parts):
        heights = jax.random.uniform(jax.random.fold_in(jax.random.fold_in(stream_key, 6), dim), (parts,), jnp.float32, low / len(shards), largest / len(shards))
        return jnp.repeat(jnp.exp(heights), shape[dim] // parts).reshape((-1,) + (1,) * (len(shape) - dim - 1))

    level = one(*shards[0])
    for cut in shards[1:]:
        level = level * one(*cut)
    return level


def noise(own_key, extent, spread, bound, cuts=(), held_as=jnp.bfloat16):
    factor_of = steps_of(own_key, extent, cuts, -0.22, 0.18) if cuts else 1.0
    values = jax.random.normal(own_key, extent, jnp.float32) * spread * factor_of
    return jnp.minimum(jnp.maximum(values, -bound), bound).astype(held_as)


def setup_inputs(seed: int = 0) -> dict:
    splits = jax.random.split(jax.random.key(seed), 10)
    ham_blocks = noise(splits[0], (HBLOCKS, B, B), 0.02, 0.119628906, ((0, 256),))
    onsite = jnp.clip(jax.random.uniform(splits[1], (DEVICES, M), jnp.float32, -1.0, 1.0) * steps_of(splits[1], (DEVICES, M), ((0, 256),), -0.4, 0.0), -1.0, 1.0)
    entry_slot = draw_entry_slot(jax.random.fold_in(splits[9], 71), 0)
    send_table = draw_send_table(jax.random.fold_in(splits[9], 71), 0)
    reads = draw_reads(jax.random.fold_in(splits[9], 71), 0)
    gram_targets = draw_gram_targets(jax.random.fold_in(splits[9], 71), 0)
    table_pick = draw_table_pick(jax.random.fold_in(splits[9], 71), 0)
    phi = noise(splits[7], (DEVICES, NOV, B, G), 0.4, 2.390625, ((0, 256),))
    potential_in = noise(splits[8], (NX, NY, NZ), 0.25, 1.5, ((0, 4), (1, 8), (2, 8)), jnp.float32)
    return dict(ham_blocks=ham_blocks, onsite=onsite, entry_slot=entry_slot, send_table=send_table, reads=reads, gram_targets=gram_targets, table_pick=table_pick, phi=phi, potential_in=potential_in)


SHIFTS_X = (0, -1, 1, 0, 0, 0, 0)
SHIFTS_Y = (0, 0, 0, -1, 1, 0, 0)
SHIFTS_Z = (0, 0, 0, 0, 0, -1, 1)
EPSILON = 1e-06

def neighbour(device, face):
    plane = N_GY * N_GZ
    coord_x = device // plane
    coord_y = device // N_GZ % N_GY
    coord_z = device % N_GZ
    coord_x = (coord_x + jnp.array(SHIFTS_X, jnp.int32)[face]) % N_GX
    coord_y = (coord_y + jnp.array(SHIFTS_Y, jnp.int32)[face]) % N_GY
    coord_z = (coord_z + jnp.array(SHIFTS_Z, jnp.int32)[face]) % N_GZ
    return (coord_x * N_GY + coord_y) * N_GZ + coord_z

def assemble(device, ham_blocks, entry_slot, send_table):
    plane = N_GY * N_GZ
    positions = entry_slot[device]
    owners = device // plane * plane + positions // CAP
    chosen = send_table[owners, device % plane, positions % CAP]
    blocks = ham_blocks[owners * HB_DEV + chosen]
    return blocks.reshape(S, S, B, B).transpose(0, 2, 1, 3).reshape(M, M)

def density_columns(matrix, onsite_row):
    wide = matrix.astype(jnp.float32)
    hamilton = 0.5 * (wide + wide.T) + jnp.diag(onsite_row.astype(jnp.float32))
    factor = lax.rsqrt(jnp.sum(hamilton * hamilton) / M + EPSILON) / 1.3
    start = (hamilton * factor).astype(jnp.bfloat16)
    square = jnp.dot(start, start, preferred_element_type=jnp.float32).astype(jnp.bfloat16)
    cube = jnp.dot(start, square, preferred_element_type=jnp.float32)
    first = (1.5 * start.astype(jnp.float32) - 0.5 * cube).astype(jnp.bfloat16)
    column = first[:, :B]
    inner = jnp.dot(first, column, preferred_element_type=jnp.float32).astype(jnp.bfloat16)
    outer = jnp.dot(first, inner, preferred_element_type=jnp.float32)
    unit = (jnp.arange(M)[:, None] == jnp.arange(B)[None, :]).astype(jnp.float32)
    result = 0.5 * (unit - (1.5 * column.astype(jnp.float32) - 0.5 * outer))
    return result.astype(jnp.bfloat16).reshape(S, B, B)

def jacobi(field, source):
    beside_all = jnp.roll(field, -1, 0) + jnp.roll(field, 1, 0)
    beside_all = beside_all + jnp.roll(field, -1, 1) + jnp.roll(field, 1, 1)
    beside_all = beside_all + jnp.roll(field, -1, 2) + jnp.roll(field, 1, 2)
    return (beside_all + source) / 6.0

def reference(ham_blocks, onsite, entry_slot, send_table, reads, gram_targets, table_pick, phi, potential_in):
    plane = N_GY * N_GZ
    devices = jnp.arange(DEVICES, dtype=jnp.int32)

    def one_submatrix(device):
        return density_columns(assemble(device, ham_blocks, entry_slot, send_table), onsite[device])
    density = lax.map(one_submatrix, devices)
    candidates = jnp.concatenate([density.reshape(DEVICES * S, B, B), jnp.zeros((1, B, B), density.dtype)])

    def one_brick(device):
        codes = reads[device]
        live = codes < 7 * S
        faces = jnp.where(live, codes // S, 0)
        sources = neighbour(device, faces)
        index = jnp.where(live, sources * S + codes % S, DEVICES * S)
        blocks = candidates[index].astype(jnp.float32)
        left_table = phi[device][table_pick[device, 0]].astype(jnp.float32)
        right_table = phi[device][table_pick[device, 1]].astype(jnp.float32)
        mixed = jnp.einsum('rij,rig->rjg', blocks, left_table, precision=lax.Precision.HIGHEST)
        return lax.optimization_barrier(jnp.sum(mixed * right_table, axis=(0, 1)))
    brick_rho = lax.map(one_brick, devices)
    source = brick_rho.reshape(N_GX, N_GY, N_GZ, BX, BY, BZ).transpose(0, 3, 1, 4, 2, 5).reshape(NX, NY, NZ)
    potential = potential_in
    for sweep_index in range(2):
        potential = jacobi(potential, source)
    bricks = potential.reshape(N_GX, BX, N_GY, BY, N_GZ, BZ).transpose(0, 2, 4, 1, 3, 5).reshape(DEVICES, G)

    def one_gram(device):
        left_table = phi[device][table_pick[device, 0]].astype(jnp.float32)
        scaled = (phi[device][table_pick[device, 1]].astype(jnp.float32) * bricks[device][None, None, :]).astype(jnp.bfloat16)
        scaled = lax.optimization_barrier(scaled).astype(jnp.float32)
        return jnp.einsum('rig,rjg->rij', left_table, scaled, precision=lax.Precision.HIGHEST).astype(jnp.bfloat16)
    gram_all = lax.map(one_gram, devices)

    def one_return(device):
        sources = neighbour(device, jnp.arange(7, dtype=jnp.int32))
        pieces = gram_all[sources].reshape(7 * RMAX, B, B).astype(jnp.float32)
        selector = (gram_targets[device].reshape(-1)[None, :] == jnp.arange(S * S, dtype=jnp.int32)[:, None]).astype(jnp.float32)
        return jnp.einsum('sq,qij->sij', selector, pieces, precision=lax.Precision.HIGHEST).astype(jnp.bfloat16)
    positions = entry_slot
    owners = devices[:, None] // plane * plane + positions // CAP
    chosen = send_table[owners, (devices % plane)[:, None], positions % CAP]
    target = (owners * HB_DEV + chosen).astype(jnp.int32)

    def add_returned(device, total):
        piece = one_return(device).astype(jnp.float32)
        return total.at[target[device]].add(piece)
    grid_blocks = lax.fori_loop(0, DEVICES, add_returned, jnp.zeros((HBLOCKS, B, B), jnp.float32))
    return (potential, grid_blocks)
```

```python
import functools

import jax
import jax.numpy as jnp
from jax import lax
from jax.experimental import pallas as pl
from jax.experimental.pallas import tpu as pltpu
from jax.sharding import PartitionSpec as P

B = 128
S = 6
M = 768
RMAX = 8
NOV = 4
EPSILON = 1e-06
SIDES = (("gx", 0), ("gy", 1), ("gz", 2))
F32 = jnp.float32
BF16 = jnp.bfloat16

SMEM = pl.BlockSpec(memory_space=pltpu.SMEM)
VMEM = pl.BlockSpec(memory_space=pltpu.VMEM)


def call(kernel, out_shape, ins, smem, scratch=(), limit=24, cost=None):
    return pl.pallas_call(
        kernel,
        out_shape=out_shape,
        in_specs=[SMEM] * smem + [VMEM] * (len(ins) - smem),
        out_specs=jax.tree.map(lambda _: VMEM, out_shape),
        scratch_shapes=list(scratch),
        compiler_params=pltpu.CompilerParams(vmem_limit_bytes=limit * 1024 * 1024),
        cost_estimate=cost,
    )(*ins)


def shape(dims, dtype):
    return jax.ShapeDtypeStruct(dims, dtype)


def outgoing_kernel(picks_ref, ham_ref, out_ref):
    def one(q, carry):
        out_ref[q] = ham_ref[jnp.maximum(picks_ref[q], 0)]
        return carry

    lax.fori_loop(0, out_ref.shape[0], one, 0, unroll=4)


def density_kernel(slots_ref, incoming_ref, onsite_ref, out_ref, h_ref, x_ref, q_ref):
    rows = lax.broadcasted_iota(jnp.int32, (B, B), 0)
    cols = lax.broadcasted_iota(jnp.int32, (B, B), 1)
    eye = rows == cols
    total = jnp.zeros((8, B), F32)

    def block(s, t):
        return incoming_ref[slots_ref[s * S + t]].astype(F32)

    for s in range(S):
        for t in range(s, S):
            if s == t:
                a = block(s, s)
                diag = onsite_ref[0:1, s * B : (s + 1) * B]
                h = 0.5 * (a + a.T) + jnp.where(eye, diag, 0.0)
                h_ref[s * B : (s + 1) * B, s * B : (s + 1) * B] = h
                total = total + jnp.sum((h * h).reshape(B // 8, 8, B), axis=0)
            else:
                h = 0.5 * (block(s, t) + block(t, s).T)
                h_ref[s * B : (s + 1) * B, t * B : (t + 1) * B] = h
                h_ref[t * B : (t + 1) * B, s * B : (s + 1) * B] = h.T
                total = total + 2.0 * jnp.sum((h * h).reshape(B // 8, 8, B), axis=0)
    norm = jnp.sum(jnp.sum(total, axis=0, keepdims=True), axis=1, keepdims=True)
    factor = lax.rsqrt(norm / M + EPSILON) / 1.3
    for s in range(S):
        x_ref[s * B : (s + 1) * B, :] = (h_ref[s * B : (s + 1) * B, :] * factor).astype(BF16)
    x0 = x_ref[...]
    for s in range(0, S, 2):
        part = slice(s * B, (s + 2) * B)
        q_ref[:, part] = jnp.dot(x0, x_ref[:, part], preferred_element_type=F32).astype(BF16)
    for s in range(0, S, 2):
        part = slice(s * B, (s + 2) * B)
        cube = jnp.dot(x0, q_ref[:, part], preferred_element_type=F32)
        h_ref[:, part] = 1.5 * x_ref[:, part].astype(F32) - 0.5 * cube
    x1 = h_ref[...].astype(BF16)
    column = x1[:, :B]
    inner = jnp.dot(x1, column, preferred_element_type=F32).astype(BF16)
    outer = jnp.dot(x1, inner, preferred_element_type=F32)
    for s in range(S):
        part = slice(s * B, (s + 1) * B)
        value = 1.5 * column[part].astype(F32) - 0.5 * outer[part]
        if s == 0:
            value = jnp.where(eye, 1.0, 0.0) - value
        else:
            value = 0.0 - value
        out_ref[s] = (0.5 * value).astype(BF16)


def rho_kernel(reads_ref, pick_ref, *refs):
    faces = refs[:7]
    phi_ref, rho_ref, p_ref = refs[7:]
    p_ref[...] = jnp.zeros(p_ref.shape, F32)

    def slot(r, carry):
        code = reads_ref[r]
        row = pl.multiple_of(pick_ref[r] * B, B)
        right = pick_ref[RMAX + r]
        for k in range(7):

            @pl.when((code >= k * S) & (code < (k + 1) * S))
            def _():
                at = (right, pl.ds(row, B))
                p_ref[at] = p_ref[at] + faces[k][code - k * S].astype(F32)

        return carry

    lax.fori_loop(0, RMAX, slot, 0)
    pc = jnp.concatenate([p_ref[t].astype(BF16) for t in range(NOV)], axis=1)
    width = 512
    for c in range(phi_ref.shape[1] // width):
        part = phi_ref[:, c * width : (c + 1) * width]
        mixed = jnp.dot(pc, part, preferred_element_type=F32)
        value = mixed * part.astype(F32)
        value = jnp.sum(value.reshape(NOV * B // 8, 8, width), axis=0)
        value = jnp.sum(value, axis=0, keepdims=True)
        for k in range(width // B):
            row = c * (width // B) + k
            rho_ref[row : row + 1, :] = value[:, k * B : (k + 1) * B]


def gram_kernel(pick_ref, v_ref, phi_ref, out_ref, w_ref, g_ref):
    for k in range(v_ref.shape[0]):
        part = slice(k * B, (k + 1) * B)
        w_ref[:, part] = (phi_ref[:, part].astype(F32) * v_ref[k : k + 1, :]).astype(BF16)
    for t in range(0, NOV, 2):
        g = lax.dot_general(
            phi_ref[...],
            w_ref[t * B : (t + 2) * B, :],
            (((1,), (1,)), ((), ())),
            preferred_element_type=F32,
        )
        g_ref[t] = g[:, :B]
        g_ref[t + 1] = g[:, B:]

    def slot(r, carry):
        row = pl.multiple_of(pick_ref[r] * B, B)
        out_ref[r] = g_ref[pick_ref[RMAX + r], pl.ds(row, B)].astype(BF16)
        return carry

    lax.fori_loop(0, RMAX, slot, 0)


def return_kernel(targets_ref, slots_ref, *refs):
    faces = refs[:7]
    out_ref = refs[7]

    def clear(q, carry):
        out_ref[q] = jnp.zeros((B, B), BF16)
        return carry

    lax.fori_loop(0, out_ref.shape[0], clear, 0, unroll=4)
    for k in range(7):

        def slot(r, carry):
            target = targets_ref[k * RMAX + r]

            @pl.when(target < S * S)
            def _():
                at = slots_ref[target]
                total = out_ref[at].astype(F32) + faces[k][r].astype(F32)
                out_ref[at] = total.astype(BF16)

            return carry

        lax.fori_loop(0, RMAX, slot, 0)


def owner_kernel(picks_ref, arrived_ref, out_ref):
    out_ref[...] = jnp.zeros(out_ref.shape, F32)

    def one(q, carry):
        pick = picks_ref[q]

        @pl.when(pick >= 0)
        def _():
            out_ref[pick] = out_ref[pick] + arrived_ref[q].astype(F32)

        return carry

    lax.fori_loop(0, arrived_ref.shape[0], one, 0)


def face_exchange(x):
    out = [x]
    for axis, _ in SIDES:
        size = lax.axis_size(axis)
        up = [(i, (i + 1) % size) for i in range(size)]
        out.append(lax.ppermute(x, axis, up))
        out.append(lax.ppermute(x, axis, [(b, a) for a, b in up]))
    return out


def extended(x):
    edges = {}
    for axis, dim in SIDES:
        size, length = (lax.axis_size(axis), x.shape[dim])
        up = [(i, (i + 1) % size) for i in range(size)]
        last = lax.slice_in_dim(x, length - 1, length, axis=dim)
        first = lax.slice_in_dim(x, 0, 1, axis=dim)
        edges[dim] = (
            lax.ppermute(last, axis, up),
            lax.ppermute(first, axis, [(b, a) for a, b in up]),
        )
    done = []
    for _, dim in SIDES:
        low, high = edges[dim]
        around = [(1, 1) if d in done else (0, 0) for d in range(x.ndim)]
        x = jnp.concatenate([jnp.pad(low, around), x, jnp.pad(high, around)], axis=dim)
        done.append(dim)
    return x


def jacobi_step(padded, source):
    beside_all = padded[2:, 1:-1, 1:-1] + padded[:-2, 1:-1, 1:-1]
    beside_all = beside_all + padded[1:-1, 2:, 1:-1] + padded[1:-1, :-2, 1:-1]
    beside_all = beside_all + padded[1:-1, 1:-1, 2:] + padded[1:-1, 1:-1, :-2]
    return (beside_all + source) / 6.0


def select_outgoing(picks, ham_blocks):
    return call(outgoing_kernel, shape((picks.shape[0], B, B), BF16), (picks, ham_blocks), 1)


def density_of(slots, incoming, onsite):
    return call(
        density_kernel,
        shape((S, B, B), BF16),
        (slots, incoming, onsite),
        1,
        (pltpu.VMEM((M, M), F32), pltpu.VMEM((M, M), BF16), pltpu.VMEM((M, M), BF16)),
    )


def rho_of(codes, pick, faces, tables):
    return call(
        rho_kernel,
        shape((tables.shape[1] // B, B), F32),
        (codes, pick, *faces, tables),
        2,
        (pltpu.VMEM((NOV, NOV * B, B), F32),),
    )


def gram_of(pick, potential, tables):
    return call(
        gram_kernel,
        shape((RMAX, B, B), BF16),
        (pick, potential, tables),
        1,
        (pltpu.VMEM(tables.shape, BF16), pltpu.VMEM((NOV, NOV * B, B), F32)),
    )


def returned_of(targets, slots, grams, count):
    return call(return_kernel, shape((count, B, B), BF16), (targets, slots, *grams), 2)


def owned_of(picks, arrived, held):
    return call(owner_kernel, shape((held, B, B), F32), (picks, arrived), 1)


def shards(
    ham_blocks, onsite, entry_slot, send_table, reads, gram_targets, table_pick, phi, potential_in
):
    held = ham_blocks.shape[0]
    slot_ids = entry_slot[0]
    picks = send_table.reshape(-1)
    pick = table_pick.reshape(-1)
    tables = phi.reshape(NOV * B, -1)
    outgoing = select_outgoing(picks, ham_blocks)
    incoming = lax.all_to_all(outgoing, ("gy", "gz"), split_axis=0, concat_axis=0, tiled=True)
    density = density_of(slot_ids, incoming, onsite)
    faces = face_exchange(density)
    source = rho_of(reads[0], pick, faces, tables).reshape(potential_in.shape)
    potential = potential_in
    for sweep_index in range(2):
        potential = jacobi_step(extended(potential), source)
    grams = gram_of(pick, potential.reshape(-1, B), tables)
    outgoing_back = returned_of(
        gram_targets.reshape(-1), slot_ids, face_exchange(grams), picks.shape[0]
    )
    arrived = lax.all_to_all(outgoing_back, ("gy", "gz"), split_axis=0, concat_axis=0, tiled=True)
    return (potential, owned_of(picks, arrived, held))


def solution(mesh):
    whole = ("gx", "gy", "gz")
    placed = (
        P(whole, None, None),
        P(whole, None),
        P(whole, None),
        P(whole, None, None),
        P(whole, None),
        P(whole, None, None),
        P(whole, None, None),
        P(whole, None, None, None),
        P("gx", "gy", "gz"),
    )
    return jax.shard_map(
        shards,
        mesh=mesh,
        in_specs=placed,
        out_specs=(P("gx", "gy", "gz"), P(whole, None, None)),
        check_vma=False,
    )
```

```python
import functools

import jax
import jax.numpy as jnp
from jax import lax
from jax.experimental import pallas as pl
from jax.experimental.pallas import tpu as pltpu
from jax.sharding import PartitionSpec as P


B = 128
S = 6
M = 768
RMAX = 8
NOV = 4
EPSILON = 1e-06
N = 8
BY = 8
HELD = 8
NEAR = (0, -1, 1, -2, 2)
FAR = (-3, 3, 4)
SIDES = (("gx", 0), ("gy", 1), ("gz", 2))
F32 = jnp.float32
BF16 = jnp.bfloat16

SMEM = pl.BlockSpec(memory_space=pltpu.SMEM)
VMEM = pl.BlockSpec(memory_space=pltpu.VMEM)


def call(kernel, out_shape, ins, smem, scratch=(), limit=24, cost=None):
    return pl.pallas_call(
        kernel,
        out_shape=out_shape,
        in_specs=[SMEM] * smem + [VMEM] * (len(ins) - smem),
        out_specs=jax.tree.map(lambda _: VMEM, out_shape),
        scratch_shapes=list(scratch),
        compiler_params=pltpu.CompilerParams(vmem_limit_bytes=limit * 1024 * 1024),
        cost_estimate=cost,
    )(*ins)


def shape(dims, dtype):
    return jax.ShapeDtypeStruct(dims, dtype)


def wrapped(i):
    return lax.bitwise_and(i, N - 1)


def near_kernel(table_ref, here_ref, *refs):
    out_ref = refs[-1]
    for o, offset in enumerate(NEAR):
        row = wrapped(here_ref[0] + offset)

        def one(j, carry):
            out_ref[j, o] = refs[o][jnp.maximum(table_ref[row, 0, j], 0)]
            return carry

        lax.fori_loop(0, N, one, 0, unroll=2)


def far_kernel(table_ref, here_ref, *refs):
    sets = refs[:4]
    outs = refs[4:]
    for o, offset in enumerate(FAR):
        row = wrapped(here_ref[0] + offset)
        for step in range(N):
            pick = jnp.maximum(table_ref[row, 0, wrapped(here_ref[1] + step)], 0)
            if o < 2:
                outs[step][o] = sets[o][pick]
            else:
                half = HELD // 2
                low = sets[2][jnp.minimum(pick, half - 1)]
                high = sets[3][jnp.maximum(pick - half, 0)]
                outs[step][o] = jnp.where(pick < half, low, high)


def density_kernel(slots_ref, here_ref, *refs):
    near_ref = refs[0]
    far = refs[1 : 1 + N]
    onsite_ref, v_ref, out_ref, incoming_ref, h_ref, x_ref, q_ref = refs[1 + N :]
    for o, offset in enumerate(NEAR):

        def keep(i, carry):
            incoming_ref[(offset % N) * N + i] = near_ref[i, o]
            return carry

        lax.fori_loop(0, N, keep, 0, unroll=2)
    for step in range(N):
        i = wrapped(here_ref[1] - step)
        for o, offset in enumerate(FAR):
            incoming_ref[(offset % N) * N + i] = far[step][o]
    v = v_ref[...]
    high = v.astype(BF16)
    rest = v - high.astype(F32)
    middle = rest.astype(BF16)
    low = (rest - middle.astype(F32)).astype(BF16)
    out_ref[S] = jnp.concatenate([high, middle, low, jnp.zeros_like(low)], axis=0)
    rows = lax.broadcasted_iota(jnp.int32, (B, B), 0)
    cols = lax.broadcasted_iota(jnp.int32, (B, B), 1)
    eye = rows == cols
    total = jnp.zeros((8, B), F32)

    def block(s, t):
        slot = slots_ref[s * S + t]
        offset = wrapped(slot - here_ref[0])
        return incoming_ref[offset * N + lax.div(slot, N)].astype(F32)

    for s in range(S):
        for t in range(s, S):
            if s == t:
                a = block(s, s)
                diag = onsite_ref[0:1, s * B : (s + 1) * B]
                h = 0.5 * (a + a.T) + jnp.where(eye, diag, 0.0)
                h_ref[s * B : (s + 1) * B, s * B : (s + 1) * B] = h
                total = total + jnp.sum((h * h).reshape(B // 8, 8, B), axis=0)
            else:
                h = 0.5 * (block(s, t) + block(t, s).T)
                h_ref[s * B : (s + 1) * B, t * B : (t + 1) * B] = h
                h_ref[t * B : (t + 1) * B, s * B : (s + 1) * B] = h.T
                total = total + 2.0 * jnp.sum((h * h).reshape(B // 8, 8, B), axis=0)
    norm = jnp.sum(jnp.sum(total, axis=0, keepdims=True), axis=1, keepdims=True)
    factor = lax.rsqrt(norm / M + EPSILON) / 1.3
    for s in range(S):
        x_ref[s * B : (s + 1) * B, :] = (h_ref[s * B : (s + 1) * B, :] * factor).astype(BF16)
    x0 = x_ref[...]
    for s in range(0, S, 2):
        part = slice(s * B, (s + 2) * B)
        q_ref[:, part] = jnp.dot(x0, x_ref[:, part], preferred_element_type=F32).astype(BF16)
    for s in range(0, S, 2):
        part = slice(s * B, (s + 2) * B)
        cube = jnp.dot(x0, q_ref[:, part], preferred_element_type=F32)
        h_ref[:, part] = 1.5 * x_ref[:, part].astype(F32) - 0.5 * cube
    x1 = h_ref[...].astype(BF16)
    column = x1[:, :B]
    inner = jnp.dot(x1, column, preferred_element_type=F32).astype(BF16)
    outer = jnp.dot(x1, inner, preferred_element_type=F32)
    for s in range(S):
        part = slice(s * B, (s + 1) * B)
        value = 1.5 * column[part].astype(F32) - 0.5 * outer[part]
        if s == 0:
            value = jnp.where(eye, 1.0, 0.0) - value
        else:
            value = 0.0 - value
        out_ref[s] = (0.5 * value).astype(BF16)


def hold_kernel(phi_ref, out_ref):
    out_ref[...] = phi_ref[...]


def turn_kernel(picks_ref, out_ref):
    def one(j, carry):
        for z in range(N):
            out_ref[z, 0, j] = picks_ref[j * N + z]
        return carry

    lax.fori_loop(0, N, one, 0)


def rho_kernel(reads_ref, pick_ref, *refs):
    faces = refs[:7]
    v_ref, phi_ref, rho_ref, next_ref, p_ref = refs[7:]
    width = 512
    chunks = phi_ref.shape[1] // width
    p_ref[...] = jnp.zeros(p_ref.shape, F32)

    def slot(r, carry):
        code = reads_ref[r]
        row = pl.multiple_of(pick_ref[r] * B, B)
        right = pick_ref[RMAX + r]
        for k in range(7):

            @pl.when((code >= k * S) & (code < (k + 1) * S))
            def _():
                at = (right, pl.ds(row, B))
                p_ref[at] = p_ref[at] + faces[k][code - k * S].astype(F32)

        return carry

    lax.fori_loop(0, RMAX, slot, 0)
    pc = jnp.concatenate([p_ref[t].astype(BF16) for t in range(NOV)], axis=1)
    for c in range(chunks):
        part = phi_ref[:, c * width : (c + 1) * width]
        mixed = jnp.dot(pc, part, preferred_element_type=F32)
        value = mixed * part.astype(F32)
        value = jnp.sum(value.reshape(NOV * B // 8, 8, width), axis=0)
        value = jnp.sum(value, axis=0, keepdims=True)
        for k in range(width // B):
            row = c * (width // B) + k
            rho_ref[row : row + 1, :] = value[:, k * B : (k + 1) * B]
    v = v_ref[...]
    count = v.shape[0]

    def field(k):
        terms = [faces[k][S, t * count : (t + 1) * count].astype(F32) for t in range(3)]
        return (terms[0] + terms[1]) + terms[2]

    row = lax.broadcasted_iota(jnp.int32, v.shape, 0)
    lane = lax.broadcasted_iota(jnp.int32, v.shape, 1)
    at_y = lax.rem(row, BY)
    beside = jnp.concatenate([v[BY:], field(2)[:BY]], axis=0)
    beside = beside + jnp.concatenate([field(1)[count - BY :], v[: count - BY]], axis=0)
    beside = beside + jnp.where(
        at_y == BY - 1, pltpu.roll(field(4), BY - 1, 0), pltpu.roll(v, count - 1, 0)
    )
    beside = beside + jnp.where(
        at_y == 0, pltpu.roll(field(3), count - BY + 1, 0), pltpu.roll(v, 1, 0)
    )
    beside = beside + jnp.where(
        lane == B - 1, pltpu.roll(field(6), B - 1, 1), pltpu.roll(v, B - 1, 1)
    )
    beside = beside + jnp.where(lane == 0, pltpu.roll(field(5), 1, 1), pltpu.roll(v, 1, 1))
    next_ref[...] = (beside + rho_ref[...]) / 6.0


def gram_kernel(pick_ref, v_ref, phi_ref, out_ref, w_ref, g_ref):
    for k in range(v_ref.shape[0]):
        part = slice(k * B, (k + 1) * B)
        w_ref[:, part] = (phi_ref[:, part].astype(F32) * v_ref[k : k + 1, :]).astype(BF16)
    for t in range(0, NOV, 2):
        g = lax.dot_general(
            phi_ref[...],
            w_ref[t * B : (t + 2) * B, :],
            (((1,), (1,)), ((), ())),
            preferred_element_type=F32,
        )
        g_ref[t] = g[:, :B]
        g_ref[t + 1] = g[:, B:]

    def slot(r, carry):
        row = pl.multiple_of(pick_ref[r] * B, B)
        out_ref[r] = g_ref[pick_ref[RMAX + r], pl.ds(row, B)].astype(BF16)
        return carry

    lax.fori_loop(0, RMAX, slot, 0)


def return_kernel(targets_ref, slots_ref, here_ref, *refs):
    faces = refs[:7]
    near_ref = refs[7]
    far = refs[8 : 8 + N]
    sum_ref = refs[8 + N]

    def clear(q, carry):
        sum_ref[q] = jnp.zeros((B, B), BF16)
        return carry

    lax.fori_loop(0, sum_ref.shape[0], clear, 0, unroll=8)
    for k in range(7):

        def slot(r, carry):
            target = targets_ref[k * RMAX + r]

            @pl.when(target < S * S)
            def _():
                slot_id = slots_ref[target]
                offset = wrapped(slot_id - here_ref[0])
                at = offset * N + lax.div(slot_id, N)
                total = sum_ref[at].astype(F32) + faces[k][r].astype(F32)
                sum_ref[at] = total.astype(BF16)

            return carry

        lax.fori_loop(0, RMAX, slot, 0)
    for o, offset in enumerate(NEAR):

        def keep(i, carry):
            near_ref[i, o] = sum_ref[(offset % N) * N + i]
            return carry

        lax.fori_loop(0, N, keep, 0, unroll=2)
    for step in range(N):
        i = wrapped(here_ref[1] + step)
        for o, offset in enumerate(FAR):
            far[step][o] = sum_ref[(offset % N) * N + i]


def add_near(acc_ref, table_ref, row, near_ref, o):
    def one(j, carry):
        pick = table_ref[row, 0, j]

        @pl.when(pick >= 0)
        def _():
            acc_ref[pick] = acc_ref[pick] + near_ref[j, o].astype(F32)

        return carry

    lax.fori_loop(0, N, one, 0)


def add_far(acc_ref, table_ref, here_ref, far, o):
    row = wrapped(here_ref[0] + FAR[o])
    for step in range(N):
        pick = table_ref[row, 0, wrapped(here_ref[1] - step)]

        @pl.when(pick >= 0)
        def _():
            acc_ref[pick] = acc_ref[pick] + far[step][o].astype(F32)


def farthest_kernel(table_ref, here_ref, *refs):
    far = refs[:N]
    up_ref, down_ref, acc_ref = refs[N:]
    half = HELD // 2
    acc_ref[...] = jnp.zeros(acc_ref.shape, F32)
    add_far(acc_ref, table_ref, here_ref, far, 2)
    up_ref[...] = acc_ref[:half].astype(BF16)
    down_ref[...] = acc_ref[half:].astype(BF16)


def far_stage_kernel(o, table_ref, here_ref, *refs):
    far = refs[:N]
    handed_ref, next_ref, acc_ref = refs[N:]
    half = HELD // 2
    held = slice(half * (1 - o), half * (2 - o))
    rest = slice(half * o, half * (1 + o))
    acc_ref[rest] = jnp.zeros((half, B, B), F32)
    acc_ref[held] = handed_ref[...].astype(F32)
    add_far(acc_ref, table_ref, here_ref, far, o)
    next_ref[...] = acc_ref[...].astype(BF16)


def near_stage_kernel(o, table_ref, here_ref, near_ref, handed_ref, next_ref, acc_ref):
    acc_ref[...] = handed_ref[...].astype(F32)
    add_near(acc_ref, table_ref, wrapped(here_ref[0] + NEAR[o]), near_ref, o)
    next_ref[...] = acc_ref[...].astype(BF16)


def owner_kernel(table_ref, here_ref, near_ref, up_ref, down_ref, out_ref):
    out_ref[...] = up_ref[...].astype(F32) + down_ref[...].astype(F32)
    add_near(out_ref, table_ref, here_ref[0], near_ref, 0)


def face_exchange(x):
    out = [x]
    for axis, _ in SIDES:
        size = lax.axis_size(axis)
        up = [(i, (i + 1) % size) for i in range(size)]
        out.append(lax.ppermute(x, axis, up))
        out.append(lax.ppermute(x, axis, [(b, a) for a, b in up]))
    return out


def extended(x):
    edges = {}
    for axis, dim in SIDES:
        size, length = (lax.axis_size(axis), x.shape[dim])
        up = [(i, (i + 1) % size) for i in range(size)]
        last = lax.slice_in_dim(x, length - 1, length, axis=dim)
        first = lax.slice_in_dim(x, 0, 1, axis=dim)
        edges[dim] = (
            lax.ppermute(last, axis, up),
            lax.ppermute(first, axis, [(b, a) for a, b in up]),
        )
    done = []
    for _, dim in SIDES:
        low, high = edges[dim]
        around = [(1, 1) if d in done else (0, 0) for d in range(x.ndim)]
        x = jnp.concatenate([jnp.pad(low, around), x, jnp.pad(high, around)], axis=dim)
        done.append(dim)
    return x


def jacobi_step(padded, source):
    beside_all = padded[2:, 1:-1, 1:-1] + padded[:-2, 1:-1, 1:-1]
    beside_all = beside_all + padded[1:-1, 2:, 1:-1] + padded[1:-1, :-2, 1:-1]
    beside_all = beside_all + padded[1:-1, 1:-1, 2:] + padded[1:-1, 1:-1, :-2]
    return (beside_all + source) / 6.0


def density_of(slots, here, near, far, onsite, field):
    return call(
        density_kernel,
        shape((S + 1, B, B), BF16),
        (slots, here, near, *far, onsite, field),
        2,
        (
            pltpu.VMEM((N * N, B, B), BF16),
            pltpu.VMEM((M, M), F32),
            pltpu.VMEM((M, M), BF16),
            pltpu.VMEM((M, M), BF16),
        ),
    )


def rho_of(codes, pick, faces, field, tables):
    flat = (tables.shape[1] // B, B)
    out = (shape(flat, F32), shape(flat, F32))
    ins = (codes, pick, *faces, field, tables)
    return call(rho_kernel, out, ins, 2, (pltpu.VMEM((NOV, NOV * B, B), F32),))


def gram_of(pick, potential, tables):
    return call(
        gram_kernel,
        shape((RMAX, B, B), BF16),
        (pick, potential, tables),
        1,
        (pltpu.VMEM(tables.shape, BF16), pltpu.VMEM((NOV, NOV * B, B), F32)),
    )


def returned_of(targets, slots, here, grams):
    out = (shape((N, len(NEAR), B, B), BF16),) + (shape((len(FAR), B, B), BF16),) * N
    ins = (targets, slots, here, *grams)
    out = call(return_kernel, out, ins, 3, (pltpu.VMEM((N * N, B, B), BF16),))
    return out[0], out[1:]


def ring(step):
    size = lax.axis_size("gz")
    return [(i, (i + step) % size) for i in range(size)]


def both_ways(up, down):
    return (lax.ppermute(up, "gz", ring(1)), lax.ppermute(down, "gz", ring(-1)))


def across(x):
    return lax.all_to_all(x, "gy", split_axis=0, concat_axis=0, tiled=True)


def hand_over(far):
    size = lax.axis_size("gy")
    out = [far[0]]
    for step in range(1, size):
        out.append(lax.ppermute(far[step], "gy", [(i, (i + step) % size) for i in range(size)]))
    return out


def fetched(table, here, ham_blocks):
    half = HELD // 2
    up1, down1 = both_ways(ham_blocks, ham_blocks)
    up2, down2 = both_ways(up1, down1)
    up3, down3 = both_ways(up2, down2)
    up4, down4 = both_ways(up3[:half], down3[half:])
    ins = (table, here, ham_blocks, up1, down1, up2, down2)
    near = call(near_kernel, shape((N, len(NEAR), B, B), BF16), ins, 2)
    near = across(near)
    ins = (table, here, up3, down3, up4, down4)
    far = call(far_kernel, (shape((len(FAR), B, B), BF16),) * N, ins, 2)
    far = hand_over(far)
    return near, far


def brought_back(table, here, near, far):
    acc = (pltpu.VMEM((HELD, B, B), F32),)
    part = (shape((HELD // 2, B, B), BF16),) * 2
    whole = shape((HELD, B, B), BF16)
    far = hand_over(far)
    near = across(near)
    up, down = call(farthest_kernel, part, (table, here, *far), 2, acc)
    up, down = both_ways(up, down)
    kernel = functools.partial(far_stage_kernel, 1)
    up = call(kernel, whole, (table, here, *far, up), 2, acc)
    kernel = functools.partial(far_stage_kernel, 0)
    down = call(kernel, whole, (table, here, *far, down), 2, acc)
    for stage in (2, 1):
        up, down = both_ways(up, down)
        kernel = functools.partial(near_stage_kernel, 2 * stage)
        up = call(kernel, whole, (table, here, near, up), 2, acc)
        kernel = functools.partial(near_stage_kernel, 2 * stage - 1)
        down = call(kernel, whole, (table, here, near, down), 2, acc)
    up, down = both_ways(up, down)
    ins = (table, here, near, up, down)
    return call(owner_kernel, shape((HELD, B, B), F32), ins, 2)


def shards(
    ham_blocks, onsite, entry_slot, send_table, reads, gram_targets, table_pick, phi, potential_in
):
    slot_ids = entry_slot[0]
    pick = table_pick.reshape(-1)
    tables = phi.reshape(NOV * B, -1)
    tables = call(hold_kernel, shape(tables.shape, BF16), (tables,), 0)
    field = potential_in.reshape(-1, B)
    here = jnp.stack([lax.axis_index("gz"), lax.axis_index("gy")]).astype(jnp.int32)
    sent = pl.pallas_call(
        turn_kernel, out_shape=shape((N, 1, N), jnp.int32), in_specs=[SMEM], out_specs=SMEM
    )(send_table.reshape(-1))
    table = lax.all_to_all(sent, "gz", split_axis=0, concat_axis=0, tiled=True)
    near, far = fetched(table, here, ham_blocks)
    density = density_of(slot_ids, here, near, far, onsite, field)
    faces = face_exchange(density)
    source, first = rho_of(reads[0], pick, faces, field, tables)
    dims = potential_in.shape
    potential = jacobi_step(extended(first.reshape(dims)), source.reshape(dims))
    grams = gram_of(pick, potential.reshape(-1, B), tables)
    near, far = returned_of(gram_targets.reshape(-1), slot_ids, here, face_exchange(grams))
    return (potential, brought_back(table, here, near, far))


def solution(mesh):
    whole = ("gx", "gy", "gz")
    placed = (
        P(whole, None, None),
        P(whole, None),
        P(whole, None),
        P(whole, None, None),
        P(whole, None),
        P(whole, None, None),
        P(whole, None, None),
        P(whole, None, None, None),
        P("gx", "gy", "gz"),
    )
    return jax.shard_map(
        shards,
        mesh=mesh,
        in_specs=placed,
        out_specs=(P("gx", "gy", "gz"), P(whole, None, None)),
        check_vma=False,
    )
```

```python
import functools

import jax
import jax.numpy as jnp
from jax import lax
from jax.experimental import pallas as pl
from jax.experimental.pallas import tpu as pltpu
from jax.sharding import PartitionSpec as P


B = 128
S = 6
M = 768
RMAX = 8
NOV = 4
EPSILON = 1e-06
N = 8
BY = 8
HELD = 8
NEAR = (0, -1, 1, -2, 2)
FAR = (-3, 3, 4)
SIDES = (("gx", 0), ("gy", 1), ("gz", 2))
F32 = jnp.float32
BF16 = jnp.bfloat16

SMEM = pl.BlockSpec(memory_space=pltpu.SMEM)
VMEM = pl.BlockSpec(memory_space=pltpu.VMEM)


def call(kernel, out_shape, ins, smem, scratch=(), limit=24, cost=None):
    return pl.pallas_call(
        kernel,
        out_shape=out_shape,
        in_specs=[SMEM] * smem + [VMEM] * (len(ins) - smem),
        out_specs=jax.tree.map(lambda _: VMEM, out_shape),
        scratch_shapes=list(scratch),
        compiler_params=pltpu.CompilerParams(vmem_limit_bytes=limit * 1024 * 1024),
        cost_estimate=cost,
    )(*ins)


def shape(dims, dtype):
    return jax.ShapeDtypeStruct(dims, dtype)


def wrapped(i):
    return lax.bitwise_and(i, N - 1)


def near_kernel(table_ref, here_ref, *refs):
    out_ref = refs[-1]
    for o, offset in enumerate(NEAR):
        row = wrapped(here_ref[0] + offset)

        def one(j, carry):
            out_ref[j, o] = refs[o][jnp.maximum(table_ref[row, 0, j], 0)]
            return carry

        lax.fori_loop(0, N, one, 0, unroll=2)


def far_kernel(table_ref, here_ref, *refs):
    sets = refs[: len(FAR)]
    own = refs[len(FAR) : len(FAR) + N // 2]
    other_ref = refs[len(FAR) + N // 2]
    for o, offset in enumerate(FAR):
        row = wrapped(here_ref[0] + offset)
        for step in range(N // 2):
            y = wrapped(here_ref[1] + 2 * step)
            own[step][o] = sets[o][jnp.maximum(table_ref[row, 0, y], 0)]
            other = jnp.maximum(table_ref[row, 0, y ^ 1], 0)
            other_ref[step * len(FAR) + o] = sets[o][other]


def density_kernel(slots_ref, here_ref, *refs):
    near_ref = refs[0]
    far = refs[1 : 1 + N // 2]
    onsite_ref, v_ref, out_ref, incoming_ref, h_ref, x_ref, q_ref = refs[1 + N // 2 :]
    for o, offset in enumerate(NEAR):

        def keep(i, carry):
            incoming_ref[(offset % N) * N + i] = near_ref[i, o]
            return carry

        lax.fori_loop(0, N, keep, 0, unroll=2)
    for step in range(N // 2):
        i = wrapped(here_ref[1] - 2 * step)
        for o, offset in enumerate(FAR):
            incoming_ref[(offset % N) * N + i] = far[step][o]
            incoming_ref[(offset % N) * N + (i ^ 1)] = far[step][len(FAR) + o]
    v = v_ref[...]
    high = v.astype(BF16)
    rest = v - high.astype(F32)
    middle = rest.astype(BF16)
    low = (rest - middle.astype(F32)).astype(BF16)
    out_ref[S] = jnp.concatenate([high, middle, low, jnp.zeros_like(low)], axis=0)
    rows = lax.broadcasted_iota(jnp.int32, (B, B), 0)
    cols = lax.broadcasted_iota(jnp.int32, (B, B), 1)
    eye = rows == cols
    total = jnp.zeros((8, B), F32)

    def block(s, t):
        slot = slots_ref[s * S + t]
        offset = wrapped(slot - here_ref[0])
        return incoming_ref[offset * N + lax.div(slot, N)].astype(F32)

    for s in range(S):
        for t in range(s, S):
            if s == t:
                a = block(s, s)
                diag = onsite_ref[0:1, s * B : (s + 1) * B]
                h = 0.5 * (a + a.T) + jnp.where(eye, diag, 0.0)
                h_ref[s * B : (s + 1) * B, s * B : (s + 1) * B] = h
                total = total + jnp.sum((h * h).reshape(B // 8, 8, B), axis=0)
            else:
                h = 0.5 * (block(s, t) + block(t, s).T)
                h_ref[s * B : (s + 1) * B, t * B : (t + 1) * B] = h
                h_ref[t * B : (t + 1) * B, s * B : (s + 1) * B] = h.T
                total = total + 2.0 * jnp.sum((h * h).reshape(B // 8, 8, B), axis=0)
    norm = jnp.sum(jnp.sum(total, axis=0, keepdims=True), axis=1, keepdims=True)
    factor = lax.rsqrt(norm / M + EPSILON) / 1.3

    def scaled(s, carry):
        part = pl.ds(pl.multiple_of(s * B, B), B)
        x_ref[part, :] = (h_ref[part, :] * factor).astype(BF16)
        return carry

    lax.fori_loop(0, S, scaled, 0)
    x0 = x_ref[...]
    for s in range(0, S, 2):
        part = slice(s * B, (s + 2) * B)
        q_ref[:, part] = jnp.dot(x0, x_ref[:, part], preferred_element_type=F32).astype(BF16)
    for s in range(0, S, 2):
        part = slice(s * B, (s + 2) * B)
        cube = jnp.dot(x0, q_ref[:, part], preferred_element_type=F32)
        h_ref[:, part] = 1.5 * x_ref[:, part].astype(F32) - 0.5 * cube
    x1 = h_ref[...].astype(BF16)
    column = x1[:, :B]
    inner = jnp.dot(x1, column, preferred_element_type=F32).astype(BF16)
    outer = jnp.dot(x1, inner, preferred_element_type=F32)
    for s in range(S):
        part = slice(s * B, (s + 1) * B)
        value = 1.5 * column[part].astype(F32) - 0.5 * outer[part]
        if s == 0:
            value = jnp.where(eye, 1.0, 0.0) - value
        else:
            value = 0.0 - value
        out_ref[s] = (0.5 * value).astype(BF16)


def hold_kernel(phi_ref, out_ref):
    out_ref[...] = phi_ref[...]


def turn_kernel(picks_ref, out_ref):
    def one(j, carry):
        for z in range(N):
            out_ref[z, 0, j] = picks_ref[j * N + z]
        return carry

    lax.fori_loop(0, N, one, 0)


def rho_kernel(reads_ref, pick_ref, *refs):
    faces = refs[:7]
    v_ref, phi_ref, rho_ref, next_ref, p_ref = refs[7:]
    width = 512
    chunks = phi_ref.shape[1] // width
    p_ref[...] = jnp.zeros(p_ref.shape, F32)

    def slot(r, carry):
        code = reads_ref[r]
        row = pl.multiple_of(pick_ref[r] * B, B)
        right = pick_ref[RMAX + r]
        for k in range(7):

            @pl.when((code >= k * S) & (code < (k + 1) * S))
            def _():
                at = (right, pl.ds(row, B))
                p_ref[at] = p_ref[at] + faces[k][code - k * S].astype(F32)

        return carry

    lax.fori_loop(0, RMAX, slot, 0)
    pc = jnp.concatenate([p_ref[t].astype(BF16) for t in range(NOV)], axis=1)

    def some(i, carry):
        for c in range(2):
            c = i * 2 + c
            part = phi_ref[:, pl.ds(pl.multiple_of(c * width, width), width)]
            mixed = jnp.dot(pc, part, preferred_element_type=F32)
            value = mixed * part.astype(F32)
            value = jnp.sum(value.reshape(NOV * B // 8, 8, width), axis=0)
            value = jnp.sum(value, axis=0, keepdims=True)
            for k in range(width // B):
                rho_ref[pl.ds(c * (width // B) + k, 1), :] = value[:, k * B : (k + 1) * B]
        return carry

    lax.fori_loop(0, chunks // 2, some, 0)
    v = v_ref[...]
    count = v.shape[0]

    def field(k):
        terms = [faces[k][S, t * count : (t + 1) * count].astype(F32) for t in range(3)]
        return (terms[0] + terms[1]) + terms[2]

    row = lax.broadcasted_iota(jnp.int32, v.shape, 0)
    lane = lax.broadcasted_iota(jnp.int32, v.shape, 1)
    at_y = lax.rem(row, BY)
    beside = jnp.concatenate([v[BY:], field(2)[:BY]], axis=0)
    beside = beside + jnp.concatenate([field(1)[count - BY :], v[: count - BY]], axis=0)
    beside = beside + jnp.where(
        at_y == BY - 1, pltpu.roll(field(4), BY - 1, 0), pltpu.roll(v, count - 1, 0)
    )
    beside = beside + jnp.where(
        at_y == 0, pltpu.roll(field(3), count - BY + 1, 0), pltpu.roll(v, 1, 0)
    )
    beside = beside + jnp.where(
        lane == B - 1, pltpu.roll(field(6), B - 1, 1), pltpu.roll(v, B - 1, 1)
    )
    beside = beside + jnp.where(lane == 0, pltpu.roll(field(5), 1, 1), pltpu.roll(v, 1, 1))
    next_ref[...] = (beside + rho_ref[...]) / 6.0


def gram_kernel(pick_ref, v_ref, phi_ref, out_ref, w_ref, g_ref):
    for k in range(v_ref.shape[0]):
        part = slice(k * B, (k + 1) * B)
        w_ref[:, part] = (phi_ref[:, part].astype(F32) * v_ref[k : k + 1, :]).astype(BF16)
    for t in range(0, NOV, 2):
        g = lax.dot_general(
            phi_ref[...],
            w_ref[t * B : (t + 2) * B, :],
            (((1,), (1,)), ((), ())),
            preferred_element_type=F32,
        )
        g_ref[t] = g[:, :B]
        g_ref[t + 1] = g[:, B:]

    def slot(r, carry):
        row = pl.multiple_of(pick_ref[r] * B, B)
        out_ref[r] = g_ref[pick_ref[RMAX + r], pl.ds(row, B)].astype(BF16)
        return carry

    lax.fori_loop(0, RMAX, slot, 0)


def return_kernel(targets_ref, slots_ref, here_ref, *refs):
    faces = refs[:7]
    near_ref = refs[7]
    far = refs[8 : 8 + N]
    sum_ref = refs[8 + N]

    def clear(q, carry):
        sum_ref[q] = jnp.zeros((B, B), BF16)
        return carry

    lax.fori_loop(0, sum_ref.shape[0], clear, 0, unroll=8)
    for k in range(7):

        def slot(r, carry):
            target = targets_ref[k * RMAX + r]

            @pl.when(target < S * S)
            def _():
                slot_id = slots_ref[target]
                offset = wrapped(slot_id - here_ref[0])
                at = offset * N + lax.div(slot_id, N)
                total = sum_ref[at].astype(F32) + faces[k][r].astype(F32)
                sum_ref[at] = total.astype(BF16)

            return carry

        lax.fori_loop(0, RMAX, slot, 0)
    for o, offset in enumerate(NEAR):

        def keep(i, carry):
            near_ref[i, o] = sum_ref[(offset % N) * N + i]
            return carry

        lax.fori_loop(0, N, keep, 0, unroll=2)
    for step in range(N):
        i = wrapped(here_ref[1] + step)
        for o, offset in enumerate(FAR):
            far[step][o] = sum_ref[(offset % N) * N + i]


def add_near(acc_ref, table_ref, row, near_ref, o):
    def one(j, carry):
        pick = table_ref[row, 0, j]

        @pl.when(pick >= 0)
        def _():
            acc_ref[pick] = acc_ref[pick] + near_ref[j, o].astype(F32)

        return carry

    lax.fori_loop(0, N, one, 0)


def add_far(acc_ref, table_ref, here_ref, far, o):
    row = wrapped(here_ref[0] + FAR[o])
    for step in range(N):
        pick = table_ref[row, 0, wrapped(here_ref[1] - step)]

        @pl.when(pick >= 0)
        def _():
            acc_ref[pick] = acc_ref[pick] + far[step][o].astype(F32)


def farthest_kernel(table_ref, here_ref, *refs):
    far = refs[:N]
    up_ref, acc_ref = refs[N:]
    acc_ref[...] = jnp.zeros(acc_ref.shape, F32)
    add_far(acc_ref, table_ref, here_ref, far, 2)
    up_ref[...] = acc_ref[...].astype(BF16)


def far_stage_kernel(o, table_ref, here_ref, *refs):
    far = refs[:N]
    next_ref, acc_ref = refs[-2:]
    if len(refs) > N + 2:
        acc_ref[...] = refs[N][...].astype(F32)
    else:
        acc_ref[...] = jnp.zeros(acc_ref.shape, F32)
    add_far(acc_ref, table_ref, here_ref, far, o)
    next_ref[...] = acc_ref[...].astype(BF16)


def near_stage_kernel(o, table_ref, here_ref, near_ref, handed_ref, next_ref, acc_ref):
    acc_ref[...] = handed_ref[...].astype(F32)
    add_near(acc_ref, table_ref, wrapped(here_ref[0] + NEAR[o]), near_ref, o)
    next_ref[...] = acc_ref[...].astype(BF16)


def owner_kernel(table_ref, here_ref, near_ref, up_ref, down_ref, out_ref):
    out_ref[...] = up_ref[...].astype(F32) + down_ref[...].astype(F32)
    add_near(out_ref, table_ref, here_ref[0], near_ref, 0)


def face_exchange(x):
    out = [x]
    for axis, _ in SIDES:
        size = lax.axis_size(axis)
        up = [(i, (i + 1) % size) for i in range(size)]
        out.append(lax.ppermute(x, axis, up))
        out.append(lax.ppermute(x, axis, [(b, a) for a, b in up]))
    return out


def extended(x):
    edges = {}
    for axis, dim in SIDES:
        size, length = (lax.axis_size(axis), x.shape[dim])
        up = [(i, (i + 1) % size) for i in range(size)]
        last = lax.slice_in_dim(x, length - 1, length, axis=dim)
        first = lax.slice_in_dim(x, 0, 1, axis=dim)
        edges[dim] = (
            lax.ppermute(last, axis, up),
            lax.ppermute(first, axis, [(b, a) for a, b in up]),
        )
    done = []
    for _, dim in SIDES:
        low, high = edges[dim]
        around = [(1, 1) if d in done else (0, 0) for d in range(x.ndim)]
        x = jnp.concatenate([jnp.pad(low, around), x, jnp.pad(high, around)], axis=dim)
        done.append(dim)
    return x


def jacobi_step(padded, source):
    beside_all = padded[2:, 1:-1, 1:-1] + padded[:-2, 1:-1, 1:-1]
    beside_all = beside_all + padded[1:-1, 2:, 1:-1] + padded[1:-1, :-2, 1:-1]
    beside_all = beside_all + padded[1:-1, 1:-1, 2:] + padded[1:-1, 1:-1, :-2]
    return (beside_all + source) / 6.0


FAR_OUT = (shape((len(FAR), B, B), BF16),) * (N // 2)
FAR_OUT = FAR_OUT + (shape((N // 2 * len(FAR), B, B), BF16),)


def density_of(slots, here, near, far, onsite, field):
    return call(
        density_kernel,
        shape((S + 1, B, B), BF16),
        (slots, here, near, *far, onsite, field),
        2,
        (
            pltpu.VMEM((N * N, B, B), BF16),
            pltpu.VMEM((M, M), F32),
            pltpu.VMEM((M, M), BF16),
            pltpu.VMEM((M, M), BF16),
        ),
    )


def rho_of(codes, pick, faces, field, tables):
    flat = (tables.shape[1] // B, B)
    out = (shape(flat, F32), shape(flat, F32))
    ins = (codes, pick, *faces, field, tables)
    return call(rho_kernel, out, ins, 2, (pltpu.VMEM((NOV, NOV * B, B), F32),))


def gram_of(pick, potential, tables):
    return call(
        gram_kernel,
        shape((RMAX, B, B), BF16),
        (pick, potential, tables),
        1,
        (pltpu.VMEM(tables.shape, BF16), pltpu.VMEM((NOV, NOV * B, B), F32)),
    )


def returned_of(targets, slots, here, grams):
    out = (shape((N, len(NEAR), B, B), BF16),) + (shape((len(FAR), B, B), BF16),) * N
    ins = (targets, slots, here, *grams)
    out = call(return_kernel, out, ins, 3, (pltpu.VMEM((N * N, B, B), BF16),))
    return out[0], out[1:]


def ring(step):
    size = lax.axis_size("gz")
    return [(i, (i + step) % size) for i in range(size)]


def both_ways(up, down):
    return (lax.ppermute(up, "gz", ring(1)), lax.ppermute(down, "gz", ring(-1)))


def across(x):
    return lax.all_to_all(x, "gy", split_axis=0, concat_axis=0, tiled=True)


def hand_over(far):
    size = lax.axis_size("gy")
    swapped = lax.ppermute(far[-1], "gy", [(i, i ^ 1) for i in range(size)])
    out = []
    for step, own in enumerate(far[:-1]):
        both = jnp.concatenate([own, swapped[step * len(FAR) : (step + 1) * len(FAR)]])
        if step:
            pairs = [(i, (i + 2 * step) % size) for i in range(size)]
            both = lax.ppermute(both, "gy", pairs)
        out.append(both)
    return out


def hand_back(far):
    size = lax.axis_size("gy")
    out = [far[0]]
    for step in range(1, size):
        out.append(lax.ppermute(far[step], "gy", [(i, (i + step) % size) for i in range(size)]))
    return out


def fetched(table, here, ham_blocks):
    up1, down1 = both_ways(ham_blocks, ham_blocks)
    up2, down2 = both_ways(up1, down1)
    up3, down3 = both_ways(up2, down2)
    up4 = lax.ppermute(up3, "gz", ring(1))
    ins = (table, here, ham_blocks, up1, down1, up2, down2)
    near = call(near_kernel, shape((N, len(NEAR), B, B), BF16), ins, 2)
    near = across(near)
    ins = (table, here, up3, down3, up4)
    far = call(far_kernel, FAR_OUT, ins, 2)
    far = hand_over(far)
    return near, far


def brought_back(table, here, near, far):
    acc = (pltpu.VMEM((HELD, B, B), F32),)
    whole = shape((HELD, B, B), BF16)
    far = hand_back(far)
    near = across(near)
    up = call(farthest_kernel, whole, (table, here, *far), 2, acc)
    up = lax.ppermute(up, "gz", ring(1))
    down = call(functools.partial(far_stage_kernel, 0), whole, (table, here, *far), 2, acc)
    kernel = functools.partial(far_stage_kernel, 1)
    up = call(kernel, whole, (table, here, *far, up), 2, acc)
    for stage in (2, 1):
        up, down = both_ways(up, down)
        kernel = functools.partial(near_stage_kernel, 2 * stage)
        up = call(kernel, whole, (table, here, near, up), 2, acc)
        kernel = functools.partial(near_stage_kernel, 2 * stage - 1)
        down = call(kernel, whole, (table, here, near, down), 2, acc)
    up, down = both_ways(up, down)
    ins = (table, here, near, up, down)
    return call(owner_kernel, shape((HELD, B, B), F32), ins, 2)


def shards(
    ham_blocks, onsite, entry_slot, send_table, reads, gram_targets, table_pick, phi, potential_in
):
    slot_ids = entry_slot[0]
    pick = table_pick.reshape(-1)
    tables = phi.reshape(NOV * B, -1)
    tables = call(hold_kernel, shape(tables.shape, BF16), (tables,), 0)
    field = potential_in.reshape(-1, B)
    here = jnp.stack([lax.axis_index("gz"), lax.axis_index("gy")]).astype(jnp.int32)
    sent = pl.pallas_call(
        turn_kernel, out_shape=shape((N, 1, N), jnp.int32), in_specs=[SMEM], out_specs=SMEM
    )(send_table.reshape(-1))
    table = lax.all_to_all(sent, "gz", split_axis=0, concat_axis=0, tiled=True)
    near, far = fetched(table, here, ham_blocks)
    density = density_of(slot_ids, here, near, far, onsite, field)
    faces = face_exchange(density)
    source, first = rho_of(reads[0], pick, faces, field, tables)
    dims = potential_in.shape
    potential = jacobi_step(extended(first.reshape(dims)), source.reshape(dims))
    grams = gram_of(pick, potential.reshape(-1, B), tables)
    near, far = returned_of(gram_targets.reshape(-1), slot_ids, here, face_exchange(grams))
    return (potential, brought_back(table, here, near, far))


def solution(mesh):
    whole = ("gx", "gy", "gz")
    placed = (
        P(whole, None, None),
        P(whole, None),
        P(whole, None),
        P(whole, None, None),
        P(whole, None),
        P(whole, None, None),
        P(whole, None, None),
        P(whole, None, None, None),
        P("gx", "gy", "gz"),
    )
    return jax.shard_map(
        shards,
        mesh=mesh,
        in_specs=placed,
        out_specs=(P("gx", "gy", "gz"), P(whole, None, None)),
        check_vma=False,
    )
```

```python
import functools

import jax
import jax.numpy as jnp
from jax import lax
from jax.experimental import pallas as pl
from jax.experimental.pallas import tpu as pltpu
from jax.sharding import PartitionSpec as P


B = 128
S = 6
M = 768
RMAX = 8
NOV = 4
EPSILON = 1e-06
N = 8
BY = 8
HELD = 8
NEAR = (0, -1, 1, -2, 2)
FAR = (-3, 3, 4)
EARLY = (0, 1, 2, 5, 6)
LATE = (3, 4)
SIDES = (("gx", 0), ("gy", 1), ("gz", 2))
F32 = jnp.float32
BF16 = jnp.bfloat16

SMEM = pl.BlockSpec(memory_space=pltpu.SMEM)
VMEM = pl.BlockSpec(memory_space=pltpu.VMEM)


def call(kernel, out_shape, ins, smem, scratch=(), limit=24, cost=None):
    return pl.pallas_call(
        kernel,
        out_shape=out_shape,
        in_specs=[SMEM] * smem + [VMEM] * (len(ins) - smem),
        out_specs=jax.tree.map(lambda _: VMEM, out_shape),
        scratch_shapes=list(scratch),
        compiler_params=pltpu.CompilerParams(vmem_limit_bytes=limit * 1024 * 1024),
        cost_estimate=cost,
    )(*ins)


def shape(dims, dtype):
    return jax.ShapeDtypeStruct(dims, dtype)


def wrapped(i):
    return lax.bitwise_and(i, N - 1)


def near_kernel(table_ref, here_ref, *refs):
    out_ref = refs[-1]
    for o, offset in enumerate(NEAR):
        row = wrapped(here_ref[0] + offset)

        def one(j, carry):
            out_ref[j, o] = refs[o][jnp.maximum(table_ref[row, 0, j], 0)]
            return carry

        lax.fori_loop(0, N, one, 0, unroll=2)


def far_kernel(table_ref, here_ref, *refs):
    sets = refs[: len(FAR)]
    own = refs[len(FAR) : len(FAR) + N // 2]
    other_ref = refs[len(FAR) + N // 2]
    for o, offset in enumerate(FAR):
        row = wrapped(here_ref[0] + offset)
        for step in range(N // 2):
            y = wrapped(here_ref[1] + 2 * step)
            own[step][o] = sets[o][jnp.maximum(table_ref[row, 0, y], 0)]
            other = jnp.maximum(table_ref[row, 0, y ^ 1], 0)
            other_ref[step * len(FAR) + o] = sets[o][other]


def density_kernel(slots_ref, here_ref, *refs):
    near_ref = refs[0]
    far = refs[1 : 1 + N // 2]
    onsite_ref, v_ref, out_ref, incoming_ref, h_ref, x_ref, q_ref = refs[1 + N // 2 :]
    for o, offset in enumerate(NEAR):

        def keep(i, carry):
            incoming_ref[(offset % N) * N + i] = near_ref[i, o]
            return carry

        lax.fori_loop(0, N, keep, 0, unroll=2)
    for step in range(N // 2):
        i = wrapped(here_ref[1] - 2 * step)
        for o, offset in enumerate(FAR):
            incoming_ref[(offset % N) * N + i] = far[step][o]
            incoming_ref[(offset % N) * N + (i ^ 1)] = far[step][len(FAR) + o]
    v = v_ref[...]
    high = v.astype(BF16)
    rest = v - high.astype(F32)
    middle = rest.astype(BF16)
    low = (rest - middle.astype(F32)).astype(BF16)
    out_ref[S] = jnp.concatenate([high, middle, low, jnp.zeros_like(low)], axis=0)
    rows = lax.broadcasted_iota(jnp.int32, (B, B), 0)
    cols = lax.broadcasted_iota(jnp.int32, (B, B), 1)
    eye = rows == cols
    total = jnp.zeros((8, B), F32)

    def block(s, t):
        slot = slots_ref[s * S + t]
        offset = wrapped(slot - here_ref[0])
        return incoming_ref[offset * N + lax.div(slot, N)].astype(F32)

    for s in range(S):
        for t in range(s, S):
            if s == t:
                a = block(s, s)
                diag = onsite_ref[0:1, s * B : (s + 1) * B]
                h = 0.5 * (a + a.T) + jnp.where(eye, diag, 0.0)
                h_ref[s * B : (s + 1) * B, s * B : (s + 1) * B] = h
                total = total + jnp.sum((h * h).reshape(B // 8, 8, B), axis=0)
            else:
                h = 0.5 * (block(s, t) + block(t, s).T)
                h_ref[s * B : (s + 1) * B, t * B : (t + 1) * B] = h
                h_ref[t * B : (t + 1) * B, s * B : (s + 1) * B] = h.T
                total = total + 2.0 * jnp.sum((h * h).reshape(B // 8, 8, B), axis=0)
    norm = jnp.sum(jnp.sum(total, axis=0, keepdims=True), axis=1, keepdims=True)
    factor = lax.rsqrt(norm / M + EPSILON) / 1.3
    for s in range(S):
        x_ref[s * B : (s + 1) * B, :] = (h_ref[s * B : (s + 1) * B, :] * factor).astype(BF16)
    x0 = x_ref[...]
    for s in range(0, S, 2):
        part = slice(s * B, (s + 2) * B)
        q_ref[:, part] = jnp.dot(x0, x_ref[:, part], preferred_element_type=F32).astype(BF16)
    for s in range(0, S, 2):
        part = slice(s * B, (s + 2) * B)
        cube = jnp.dot(x0, q_ref[:, part], preferred_element_type=F32)
        h_ref[:, part] = 1.5 * x_ref[:, part].astype(F32) - 0.5 * cube
    x1 = h_ref[...].astype(BF16)
    column = x1[:, :B]
    inner = jnp.dot(x1, column, preferred_element_type=F32).astype(BF16)
    outer = jnp.dot(x1, inner, preferred_element_type=F32)
    for s in range(S):
        part = slice(s * B, (s + 1) * B)
        value = 1.5 * column[part].astype(F32) - 0.5 * outer[part]
        if s == 0:
            value = jnp.where(eye, 1.0, 0.0) - value
        else:
            value = 0.0 - value
        out_ref[s] = (0.5 * value).astype(BF16)


def hold_kernel(phi_ref, out_ref):
    out_ref[...] = phi_ref[...]


def turn_kernel(picks_ref, out_ref):
    def one(j, carry):
        for z in range(N):
            out_ref[z, 0, j] = picks_ref[j * N + z]
        return carry

    lax.fori_loop(0, N, one, 0)


def rho_kernel(reads_ref, pick_ref, *refs):
    faces = refs[:7]
    v_ref, phi_ref, rho_ref, next_ref, p_ref = refs[7:]
    width = 512
    chunks = phi_ref.shape[1] // width
    p_ref[...] = jnp.zeros(p_ref.shape, F32)

    def slot(r, carry):
        code = reads_ref[r]
        row = pl.multiple_of(pick_ref[r] * B, B)
        right = pick_ref[RMAX + r]
        for k in range(7):

            @pl.when((code >= k * S) & (code < (k + 1) * S))
            def _():
                at = (right, pl.ds(row, B))
                p_ref[at] = p_ref[at] + faces[k][code - k * S].astype(F32)

        return carry

    lax.fori_loop(0, RMAX, slot, 0)
    pc = jnp.concatenate([p_ref[t].astype(BF16) for t in range(NOV)], axis=1)

    def some(i, carry):
        for c in range(2):
            c = i * 2 + c
            part = phi_ref[:, pl.ds(pl.multiple_of(c * width, width), width)]
            mixed = jnp.dot(pc, part, preferred_element_type=F32)
            value = mixed * part.astype(F32)
            value = jnp.sum(value.reshape(NOV * B // 8, 8, width), axis=0)
            value = jnp.sum(value, axis=0, keepdims=True)
            for k in range(width // B):
                rho_ref[pl.ds(c * (width // B) + k, 1), :] = value[:, k * B : (k + 1) * B]
        return carry

    lax.fori_loop(0, chunks // 2, some, 0)
    v = v_ref[...]
    count = v.shape[0]

    def field(k):
        terms = [faces[k][S, t * count : (t + 1) * count].astype(F32) for t in range(3)]
        return (terms[0] + terms[1]) + terms[2]

    row = lax.broadcasted_iota(jnp.int32, v.shape, 0)
    lane = lax.broadcasted_iota(jnp.int32, v.shape, 1)
    at_y = lax.rem(row, BY)
    beside = jnp.concatenate([v[BY:], field(2)[:BY]], axis=0)
    beside = beside + jnp.concatenate([field(1)[count - BY :], v[: count - BY]], axis=0)
    beside = beside + jnp.where(
        at_y == BY - 1, pltpu.roll(field(4), BY - 1, 0), pltpu.roll(v, count - 1, 0)
    )
    beside = beside + jnp.where(
        at_y == 0, pltpu.roll(field(3), count - BY + 1, 0), pltpu.roll(v, 1, 0)
    )
    beside = beside + jnp.where(
        lane == B - 1, pltpu.roll(field(6), B - 1, 1), pltpu.roll(v, B - 1, 1)
    )
    beside = beside + jnp.where(lane == 0, pltpu.roll(field(5), 1, 1), pltpu.roll(v, 1, 1))
    next_ref[...] = (beside + rho_ref[...]) / 6.0


def gram_kernel(pick_ref, v_ref, phi_ref, out_ref, w_ref, g_ref):
    for k in range(v_ref.shape[0]):
        part = slice(k * B, (k + 1) * B)
        w_ref[:, part] = (phi_ref[:, part].astype(F32) * v_ref[k : k + 1, :]).astype(BF16)
    for t in range(0, NOV, 2):
        g = lax.dot_general(
            phi_ref[...],
            w_ref[t * B : (t + 2) * B, :],
            (((1,), (1,)), ((), ())),
            preferred_element_type=F32,
        )
        g_ref[t] = g[:, :B]
        g_ref[t + 1] = g[:, B:]

    def slot(r, carry):
        row = pl.multiple_of(pick_ref[r] * B, B)
        out_ref[r] = g_ref[pick_ref[RMAX + r], pl.ds(row, B)].astype(BF16)
        return carry

    lax.fori_loop(0, RMAX, slot, 0)


def add_grams(k, face_ref, targets_ref, slots_ref, here_ref, sum_ref):
    def slot(r, carry):
        target = targets_ref[k * RMAX + r]

        @pl.when(target < S * S)
        def _():
            slot_id = slots_ref[target]
            offset = wrapped(slot_id - here_ref[0])
            at = offset * N + lax.div(slot_id, N)
            total = sum_ref[at].astype(F32) + face_ref[r].astype(F32)
            sum_ref[at] = total.astype(BF16)

        return carry

    lax.fori_loop(0, RMAX, slot, 0)


def early_kernel(targets_ref, slots_ref, here_ref, *refs):
    sum_ref = refs[-1]

    def clear(q, carry):
        sum_ref[q] = jnp.zeros((B, B), BF16)
        return carry

    lax.fori_loop(0, sum_ref.shape[0], clear, 0, unroll=8)
    for k, face_ref in zip(EARLY, refs):
        add_grams(k, face_ref, targets_ref, slots_ref, here_ref, sum_ref)


def return_kernel(targets_ref, slots_ref, here_ref, early_ref, *refs):
    near_ref = refs[len(LATE)]
    far = refs[len(LATE) + 1 : len(LATE) + 1 + N]
    sum_ref = refs[-1]

    def copied(q, carry):
        sum_ref[q] = early_ref[q]
        return carry

    lax.fori_loop(0, sum_ref.shape[0], copied, 0, unroll=8)
    for k, face_ref in zip(LATE, refs):
        add_grams(k, face_ref, targets_ref, slots_ref, here_ref, sum_ref)
    for o, offset in enumerate(NEAR):

        def keep(i, carry):
            near_ref[i, o] = sum_ref[(offset % N) * N + i]
            return carry

        lax.fori_loop(0, N, keep, 0, unroll=2)
    for step in range(N):
        i = wrapped(here_ref[1] + step)
        for o, offset in enumerate(FAR):
            far[step][o] = sum_ref[(offset % N) * N + i]


def add_near(acc_ref, table_ref, row, near_ref, o):
    def one(j, carry):
        pick = table_ref[row, 0, j]

        @pl.when(pick >= 0)
        def _():
            acc_ref[pick] = acc_ref[pick] + near_ref[j, o].astype(F32)

        return carry

    lax.fori_loop(0, N, one, 0)


def add_far(acc_ref, table_ref, here_ref, far, o):
    row = wrapped(here_ref[0] + FAR[o])
    for step in range(N):
        pick = table_ref[row, 0, wrapped(here_ref[1] - step)]

        @pl.when(pick >= 0)
        def _():
            acc_ref[pick] = acc_ref[pick] + far[step][o].astype(F32)


def far_sums_kernel(chosen, table_ref, here_ref, *refs):
    far = refs[:N]
    for k, o in enumerate(chosen):
        out_ref = refs[N + k]
        out_ref[...] = jnp.zeros(out_ref.shape, F32)
        add_far(out_ref, table_ref, here_ref, far, o)


def near_sums_kernel(chosen, table_ref, here_ref, near_ref, *outs):
    for out_ref, o in zip(outs, chosen):
        out_ref[...] = jnp.zeros(out_ref.shape, F32)
        add_near(out_ref, table_ref, wrapped(here_ref[0] + NEAR[o]), near_ref, o)


def face_exchange(x):
    out = [x]
    for axis, _ in SIDES:
        size = lax.axis_size(axis)
        up = [(i, (i + 1) % size) for i in range(size)]
        out.append(lax.ppermute(x, axis, up))
        out.append(lax.ppermute(x, axis, [(b, a) for a, b in up]))
    return out


def extended(x):
    edges = {}
    for axis, dim in SIDES:
        size, length = (lax.axis_size(axis), x.shape[dim])
        up = [(i, (i + 1) % size) for i in range(size)]
        last = lax.slice_in_dim(x, length - 1, length, axis=dim)
        first = lax.slice_in_dim(x, 0, 1, axis=dim)
        edges[dim] = (
            lax.ppermute(last, axis, up),
            lax.ppermute(first, axis, [(b, a) for a, b in up]),
        )
    done = []
    for _, dim in SIDES:
        low, high = edges[dim]
        around = [(1, 1) if d in done else (0, 0) for d in range(x.ndim)]
        x = jnp.concatenate([jnp.pad(low, around), x, jnp.pad(high, around)], axis=dim)
        done.append(dim)
    return x


def jacobi_step(padded, source):
    beside_all = padded[2:, 1:-1, 1:-1] + padded[:-2, 1:-1, 1:-1]
    beside_all = beside_all + padded[1:-1, 2:, 1:-1] + padded[1:-1, :-2, 1:-1]
    beside_all = beside_all + padded[1:-1, 1:-1, 2:] + padded[1:-1, 1:-1, :-2]
    return (beside_all + source) / 6.0


FAR_OUT = (shape((len(FAR), B, B), BF16),) * (N // 2)
FAR_OUT = FAR_OUT + (shape((N // 2 * len(FAR), B, B), BF16),)


def density_of(slots, here, near, far, onsite, field):
    return call(
        density_kernel,
        shape((S + 1, B, B), BF16),
        (slots, here, near, *far, onsite, field),
        2,
        (
            pltpu.VMEM((N * N, B, B), BF16),
            pltpu.VMEM((M, M), F32),
            pltpu.VMEM((M, M), BF16),
            pltpu.VMEM((M, M), BF16),
        ),
    )


def rho_of(codes, pick, faces, field, tables):
    flat = (tables.shape[1] // B, B)
    out = (shape(flat, F32), shape(flat, F32))
    ins = (codes, pick, *faces, field, tables)
    return call(rho_kernel, out, ins, 2, (pltpu.VMEM((NOV, NOV * B, B), F32),))


def gram_of(pick, potential, tables):
    return call(
        gram_kernel,
        shape((RMAX, B, B), BF16),
        (pick, potential, tables),
        1,
        (pltpu.VMEM(tables.shape, BF16), pltpu.VMEM((NOV, NOV * B, B), F32)),
    )


def returned_of(targets, slots, here, grams):
    tables = (targets, slots, here)
    whole = shape((N * N, B, B), BF16)
    early = call(early_kernel, whole, (*tables, *(grams[k] for k in EARLY)), 3)
    out = (shape((N, len(NEAR), B, B), BF16),) + (shape((len(FAR), B, B), BF16),) * N
    ins = (*tables, early, *(grams[k] for k in LATE))
    out = call(return_kernel, out, ins, 3, (pltpu.VMEM(whole.shape, BF16),))
    return out[0], out[1:]


def ring(step):
    size = lax.axis_size("gz")
    return [(i, (i + step) % size) for i in range(size)]


def both_ways(up, down):
    return (lax.ppermute(up, "gz", ring(1)), lax.ppermute(down, "gz", ring(-1)))


def across(x):
    return lax.all_to_all(x, "gy", split_axis=0, concat_axis=0, tiled=True)


def hand_over(far):
    size = lax.axis_size("gy")
    swapped = lax.ppermute(far[-1], "gy", [(i, i ^ 1) for i in range(size)])
    out = []
    for step, own in enumerate(far[:-1]):
        both = jnp.concatenate([own, swapped[step * len(FAR) : (step + 1) * len(FAR)]])
        if step:
            pairs = [(i, (i + 2 * step) % size) for i in range(size)]
            both = lax.ppermute(both, "gy", pairs)
        out.append(both)
    return out


def hand_back(far):
    size = lax.axis_size("gy")
    out = [far[0]]
    for step in range(1, size):
        out.append(lax.ppermute(far[step], "gy", [(i, (i + step) % size) for i in range(size)]))
    return out


def fetched(table, here, ham_blocks):
    up1, down1 = both_ways(ham_blocks, ham_blocks)
    up2, down2 = both_ways(up1, down1)
    up3, down3 = both_ways(up2, down2)
    up4 = lax.ppermute(up3, "gz", ring(1))
    ins = (table, here, ham_blocks, up1, down1, up2, down2)
    near = call(near_kernel, shape((N, len(NEAR), B, B), BF16), ins, 2)
    near = across(near)
    ins = (table, here, up3, down3, up4)
    far = call(far_kernel, FAR_OUT, ins, 2)
    far = hand_over(far)
    return near, far


def brought_back(table, here, near, far):
    def sums(kernel, chosen, parts):
        out = (shape((HELD, B, B), F32),) * len(chosen)
        return call(functools.partial(kernel, chosen), out, (table, here, *parts), 2)

    far = hand_back(far)
    near = across(near)
    (up,) = sums(far_sums_kernel, (2,), far)
    up = lax.ppermute(up.astype(BF16), "gz", ring(1))
    down3, up3 = sums(far_sums_kernel, (0, 1), far)
    down = lax.ppermute(down3.astype(BF16), "gz", ring(-1))
    up = lax.ppermute((up3 + up.astype(F32)).astype(BF16), "gz", ring(1))
    down2, up2 = sums(near_sums_kernel, (3, 4), (near,))
    down = lax.ppermute((down2 + down.astype(F32)).astype(BF16), "gz", ring(-1))
    up = lax.ppermute((up2 + up.astype(F32)).astype(BF16), "gz", ring(1))
    own, down1, up1 = sums(near_sums_kernel, (0, 1, 2), (near,))
    down = lax.ppermute((down1 + down.astype(F32)).astype(BF16), "gz", ring(-1))
    up = lax.ppermute((up1 + up.astype(F32)).astype(BF16), "gz", ring(1))
    return own + down.astype(F32) + up.astype(F32)


def shards(
    ham_blocks, onsite, entry_slot, send_table, reads, gram_targets, table_pick, phi, potential_in
):
    slot_ids = entry_slot[0]
    pick = table_pick.reshape(-1)
    tables = phi.reshape(NOV * B, -1)
    tables = call(hold_kernel, shape(tables.shape, BF16), (tables,), 0)
    field = potential_in.reshape(-1, B)
    here = jnp.stack([lax.axis_index("gz"), lax.axis_index("gy")]).astype(jnp.int32)
    sent = pl.pallas_call(
        turn_kernel, out_shape=shape((N, 1, N), jnp.int32), in_specs=[SMEM], out_specs=SMEM
    )(send_table.reshape(-1))
    table = lax.all_to_all(sent, "gz", split_axis=0, concat_axis=0, tiled=True)
    near, far = fetched(table, here, ham_blocks)
    density = density_of(slot_ids, here, near, far, onsite, field)
    faces = face_exchange(density)
    source, first = rho_of(reads[0], pick, faces, field, tables)
    dims = potential_in.shape
    potential = jacobi_step(extended(first.reshape(dims)), source.reshape(dims))
    grams = gram_of(pick, potential.reshape(-1, B), tables)
    near, far = returned_of(gram_targets.reshape(-1), slot_ids, here, face_exchange(grams))
    return (potential, brought_back(table, here, near, far))


def solution(mesh):
    whole = ("gx", "gy", "gz")
    placed = (
        P(whole, None, None),
        P(whole, None),
        P(whole, None),
        P(whole, None, None),
        P(whole, None),
        P(whole, None, None),
        P(whole, None, None),
        P(whole, None, None, None),
        P("gx", "gy", "gz"),
    )
    return jax.shard_map(
        shards,
        mesh=mesh,
        in_specs=placed,
        out_specs=(P("gx", "gy", "gz"), P(whole, None, None)),
        check_vma=False,
    )
```

```python
import functools

import jax
import jax.numpy as jnp
from jax import lax
from jax.experimental import pallas as pl
from jax.experimental.pallas import tpu as pltpu
from jax.sharding import PartitionSpec as P


B = 128
S = 6
M = 768
RMAX = 8
NOV = 4
EPSILON = 1e-06
N = 8
BY = 8
HELD = 8
NEAR = (0, -1, 1, -2, 2)
FAR = (-3, 3, 4)
EARLY = (0, 1, 2, 5, 6)
LATE = (3, 4)
SIDES = (("gx", 0), ("gy", 1), ("gz", 2))
F32 = jnp.float32
BF16 = jnp.bfloat16

SMEM = pl.BlockSpec(memory_space=pltpu.SMEM)
VMEM = pl.BlockSpec(memory_space=pltpu.VMEM)


def call(kernel, out_shape, ins, smem, scratch=(), limit=24, cost=None):
    return pl.pallas_call(
        kernel,
        out_shape=out_shape,
        in_specs=[SMEM] * smem + [VMEM] * (len(ins) - smem),
        out_specs=jax.tree.map(lambda _: VMEM, out_shape),
        scratch_shapes=list(scratch),
        compiler_params=pltpu.CompilerParams(vmem_limit_bytes=limit * 1024 * 1024),
        cost_estimate=cost,
    )(*ins)


def shape(dims, dtype):
    return jax.ShapeDtypeStruct(dims, dtype)


def wrapped(i):
    return lax.bitwise_and(i, N - 1)


def near_kernel(table_ref, here_ref, *refs):
    out_ref = refs[-1]
    for o, offset in enumerate(NEAR):
        row = wrapped(here_ref[0] + offset)

        def one(j, carry):
            out_ref[j, o] = refs[o][jnp.maximum(table_ref[row, 0, j], 0)]
            return carry

        lax.fori_loop(0, N, one, 0, unroll=2)


def far_kernel(table_ref, here_ref, *refs):
    sets = refs[: len(FAR)]
    own = refs[len(FAR) : len(FAR) + N // 2]
    other_ref = refs[len(FAR) + N // 2]
    for o, offset in enumerate(FAR):
        row = wrapped(here_ref[0] + offset)
        for step in range(N // 2):
            y = wrapped(here_ref[1] + 2 * step)
            own[step][o] = sets[o][jnp.maximum(table_ref[row, 0, y], 0)]
            other = jnp.maximum(table_ref[row, 0, y ^ 1], 0)
            other_ref[step * len(FAR) + o] = sets[o][other]


def density_kernel(slots_ref, here_ref, *refs):
    near_ref = refs[0]
    far = refs[1 : 1 + N // 2]
    onsite_ref, v_ref, out_ref, incoming_ref, h_ref, x_ref, q_ref = refs[1 + N // 2 :]
    for o, offset in enumerate(NEAR):

        def keep(i, carry):
            incoming_ref[(offset % N) * N + i] = near_ref[i, o]
            return carry

        lax.fori_loop(0, N, keep, 0, unroll=2)
    for step in range(N // 2):
        i = wrapped(here_ref[1] - 2 * step)
        for o, offset in enumerate(FAR):
            incoming_ref[(offset % N) * N + i] = far[step][o]
            incoming_ref[(offset % N) * N + (i ^ 1)] = far[step][len(FAR) + o]
    v = v_ref[...]
    high = v.astype(BF16)
    rest = v - high.astype(F32)
    middle = rest.astype(BF16)
    low = (rest - middle.astype(F32)).astype(BF16)
    out_ref[S] = jnp.concatenate([high, middle, low, jnp.zeros_like(low)], axis=0)
    rows = lax.broadcasted_iota(jnp.int32, (B, B), 0)
    cols = lax.broadcasted_iota(jnp.int32, (B, B), 1)
    eye = rows == cols
    total = jnp.zeros((8, B), F32)

    def block(s, t):
        slot = slots_ref[s * S + t]
        offset = wrapped(slot - here_ref[0])
        return incoming_ref[offset * N + lax.div(slot, N)].astype(F32)

    for s in range(S):
        for t in range(s, S):
            if s == t:
                a = block(s, s)
                diag = onsite_ref[0:1, s * B : (s + 1) * B]
                h = 0.5 * (a + a.T) + jnp.where(eye, diag, 0.0)
                h_ref[s * B : (s + 1) * B, s * B : (s + 1) * B] = h
                total = total + jnp.sum((h * h).reshape(B // 8, 8, B), axis=0)
            else:
                h = 0.5 * (block(s, t) + block(t, s).T)
                h_ref[s * B : (s + 1) * B, t * B : (t + 1) * B] = h
                h_ref[t * B : (t + 1) * B, s * B : (s + 1) * B] = h.T
                total = total + 2.0 * jnp.sum((h * h).reshape(B // 8, 8, B), axis=0)
    norm = jnp.sum(jnp.sum(total, axis=0, keepdims=True), axis=1, keepdims=True)
    factor = lax.rsqrt(norm / M + EPSILON) / 1.3
    for s in range(S):
        x_ref[s * B : (s + 1) * B, :] = (h_ref[s * B : (s + 1) * B, :] * factor).astype(BF16)
    x0 = x_ref[...]
    for s in range(0, S, 2):
        part = slice(s * B, (s + 2) * B)
        q_ref[:, part] = jnp.dot(x0, x_ref[:, part], preferred_element_type=F32).astype(BF16)
    for s in range(0, S, 2):
        part = slice(s * B, (s + 2) * B)
        cube = jnp.dot(x0, q_ref[:, part], preferred_element_type=F32)
        h_ref[:, part] = 1.5 * x_ref[:, part].astype(F32) - 0.5 * cube
    x1 = h_ref[...].astype(BF16)
    column = x1[:, :B]
    inner = jnp.dot(x1, column, preferred_element_type=F32).astype(BF16)
    outer = jnp.dot(x1, inner, preferred_element_type=F32)
    for s in range(S):
        part = slice(s * B, (s + 1) * B)
        value = 1.5 * column[part].astype(F32) - 0.5 * outer[part]
        if s == 0:
            value = jnp.where(eye, 1.0, 0.0) - value
        else:
            value = 0.0 - value
        out_ref[s] = (0.5 * value).astype(BF16)


def hold_kernel(in_ref, out_ref):
    size = in_ref.shape[0] // 8

    def some(i, carry):
        part = pl.ds(pl.multiple_of(i * size, size), size)
        out_ref[part] = in_ref[part]
        return carry

    lax.fori_loop(0, 8, some, 0)


def turn_kernel(picks_ref, out_ref):
    def one(j, carry):
        for z in range(N):
            out_ref[z, 0, j] = picks_ref[j * N + z]
        return carry

    lax.fori_loop(0, N, one, 0)


def rho_kernel(reads_ref, pick_ref, *refs):
    faces = refs[:7]
    v_ref, phi_ref, rho_ref, next_ref, p_ref = refs[7:]
    width = 512
    chunks = phi_ref.shape[1] // width
    p_ref[...] = jnp.zeros(p_ref.shape, F32)

    def slot(r, carry):
        code = reads_ref[r]
        row = pl.multiple_of(pick_ref[r] * B, B)
        right = pick_ref[RMAX + r]
        for k in range(7):

            @pl.when((code >= k * S) & (code < (k + 1) * S))
            def _():
                at = (right, pl.ds(row, B))
                p_ref[at] = p_ref[at] + faces[k][code - k * S].astype(F32)

        return carry

    lax.fori_loop(0, RMAX, slot, 0)
    pc = jnp.concatenate([p_ref[t].astype(BF16) for t in range(NOV)], axis=1)

    def some(i, carry):
        for c in range(2):
            c = i * 2 + c
            part = phi_ref[:, pl.ds(pl.multiple_of(c * width, width), width)]
            mixed = jnp.dot(pc, part, preferred_element_type=F32)
            value = mixed * part.astype(F32)
            value = jnp.sum(value.reshape(NOV * B // 8, 8, width), axis=0)
            value = jnp.sum(value, axis=0, keepdims=True)
            for k in range(width // B):
                rho_ref[pl.ds(c * (width // B) + k, 1), :] = value[:, k * B : (k + 1) * B]
        return carry

    lax.fori_loop(0, chunks // 2, some, 0)
    v = v_ref[...]
    count = v.shape[0]

    def field(k):
        terms = [faces[k][S, t * count : (t + 1) * count].astype(F32) for t in range(3)]
        return (terms[0] + terms[1]) + terms[2]

    row = lax.broadcasted_iota(jnp.int32, v.shape, 0)
    lane = lax.broadcasted_iota(jnp.int32, v.shape, 1)
    at_y = lax.rem(row, BY)
    beside = jnp.concatenate([v[BY:], field(2)[:BY]], axis=0)
    beside = beside + jnp.concatenate([field(1)[count - BY :], v[: count - BY]], axis=0)
    beside = beside + jnp.where(
        at_y == BY - 1, pltpu.roll(field(4), BY - 1, 0), pltpu.roll(v, count - 1, 0)
    )
    beside = beside + jnp.where(
        at_y == 0, pltpu.roll(field(3), count - BY + 1, 0), pltpu.roll(v, 1, 0)
    )
    beside = beside + jnp.where(
        lane == B - 1, pltpu.roll(field(6), B - 1, 1), pltpu.roll(v, B - 1, 1)
    )
    beside = beside + jnp.where(lane == 0, pltpu.roll(field(5), 1, 1), pltpu.roll(v, 1, 1))
    next_ref[...] = (beside + rho_ref[...]) / 6.0


def gram_kernel(pick_ref, v_ref, phi_ref, out_ref, w_ref, g_ref):
    for k in range(v_ref.shape[0]):
        part = slice(k * B, (k + 1) * B)
        w_ref[:, part] = (phi_ref[:, part].astype(F32) * v_ref[k : k + 1, :]).astype(BF16)
    for t in range(0, NOV, 2):
        g = lax.dot_general(
            phi_ref[...],
            w_ref[t * B : (t + 2) * B, :],
            (((1,), (1,)), ((), ())),
            preferred_element_type=F32,
        )
        g_ref[t] = g[:, :B]
        g_ref[t + 1] = g[:, B:]

    def slot(r, carry):
        row = pl.multiple_of(pick_ref[r] * B, B)
        out_ref[r] = g_ref[pick_ref[RMAX + r], pl.ds(row, B)].astype(BF16)
        return carry

    lax.fori_loop(0, RMAX, slot, 0)


def add_grams(k, face_ref, targets_ref, slots_ref, here_ref, sum_ref):
    def slot(r, carry):
        target = targets_ref[k * RMAX + r]

        @pl.when(target < S * S)
        def _():
            slot_id = slots_ref[target]
            offset = wrapped(slot_id - here_ref[0])
            at = offset * N + lax.div(slot_id, N)
            total = sum_ref[at].astype(F32) + face_ref[r].astype(F32)
            sum_ref[at] = total.astype(BF16)

        return carry

    lax.fori_loop(0, RMAX, slot, 0)


def early_kernel(targets_ref, slots_ref, here_ref, *refs):
    sum_ref = refs[-1]

    def clear(q, carry):
        sum_ref[q] = jnp.zeros((B, B), BF16)
        return carry

    lax.fori_loop(0, sum_ref.shape[0], clear, 0, unroll=8)
    for k, face_ref in zip(EARLY, refs):
        add_grams(k, face_ref, targets_ref, slots_ref, here_ref, sum_ref)


def return_kernel(targets_ref, slots_ref, here_ref, early_ref, *refs):
    near_ref = refs[len(LATE)]
    far = refs[len(LATE) + 1 : len(LATE) + 1 + N]
    sum_ref = refs[-1]

    def copied(q, carry):
        sum_ref[q] = early_ref[q]
        return carry

    lax.fori_loop(0, sum_ref.shape[0], copied, 0, unroll=8)
    for k, face_ref in zip(LATE, refs):
        add_grams(k, face_ref, targets_ref, slots_ref, here_ref, sum_ref)
    for o, offset in enumerate(NEAR):

        def keep(i, carry):
            near_ref[i, o] = sum_ref[(offset % N) * N + i]
            return carry

        lax.fori_loop(0, N, keep, 0, unroll=2)
    for step in range(N):
        i = wrapped(here_ref[1] + step)
        for o, offset in enumerate(FAR):
            far[step][o] = sum_ref[(offset % N) * N + i]


def add_near(acc_ref, table_ref, row, near_ref, o):
    def one(j, carry):
        pick = table_ref[row, 0, j]

        @pl.when(pick >= 0)
        def _():
            acc_ref[pick] = acc_ref[pick] + near_ref[j, o].astype(F32)

        return carry

    lax.fori_loop(0, N, one, 0)


def add_far(acc_ref, table_ref, here_ref, far, o):
    row = wrapped(here_ref[0] + FAR[o])
    for step in range(N):
        pick = table_ref[row, 0, wrapped(here_ref[1] - step)]

        @pl.when(pick >= 0)
        def _():
            acc_ref[pick] = acc_ref[pick] + far[step][o].astype(F32)


def far_sums_kernel(chosen, table_ref, here_ref, *refs):
    far = refs[:N]
    for k, o in enumerate(chosen):
        out_ref = refs[N + k]
        out_ref[...] = jnp.zeros(out_ref.shape, F32)
        add_far(out_ref, table_ref, here_ref, far, o)


def near_sums_kernel(chosen, table_ref, here_ref, near_ref, *outs):
    for out_ref, o in zip(outs, chosen):
        out_ref[...] = jnp.zeros(out_ref.shape, F32)
        add_near(out_ref, table_ref, wrapped(here_ref[0] + NEAR[o]), near_ref, o)


def face_exchange(x):
    out = [x]
    for axis, _ in SIDES:
        size = lax.axis_size(axis)
        up = [(i, (i + 1) % size) for i in range(size)]
        out.append(lax.ppermute(x, axis, up))
        out.append(lax.ppermute(x, axis, [(b, a) for a, b in up]))
    return out


def extended(x):
    edges = {}
    for axis, dim in SIDES:
        size, length = (lax.axis_size(axis), x.shape[dim])
        up = [(i, (i + 1) % size) for i in range(size)]
        last = lax.slice_in_dim(x, length - 1, length, axis=dim)
        first = lax.slice_in_dim(x, 0, 1, axis=dim)
        edges[dim] = (
            lax.ppermute(last, axis, up),
            lax.ppermute(first, axis, [(b, a) for a, b in up]),
        )
    done = []
    for _, dim in SIDES:
        low, high = edges[dim]
        around = [(1, 1) if d in done else (0, 0) for d in range(x.ndim)]
        x = jnp.concatenate([jnp.pad(low, around), x, jnp.pad(high, around)], axis=dim)
        done.append(dim)
    return x


def jacobi_step(padded, source):
    beside_all = padded[2:, 1:-1, 1:-1] + padded[:-2, 1:-1, 1:-1]
    beside_all = beside_all + padded[1:-1, 2:, 1:-1] + padded[1:-1, :-2, 1:-1]
    beside_all = beside_all + padded[1:-1, 1:-1, 2:] + padded[1:-1, 1:-1, :-2]
    return (beside_all + source) / 6.0


FAR_OUT = (shape((len(FAR), B, B), BF16),) * (N // 2)
FAR_OUT = FAR_OUT + (shape((N // 2 * len(FAR), B, B), BF16),)


def density_of(slots, here, near, far, onsite, field):
    return call(
        density_kernel,
        shape((S + 1, B, B), BF16),
        (slots, here, near, *far, onsite, field),
        2,
        (
            pltpu.VMEM((N * N, B, B), BF16),
            pltpu.VMEM((M, M), F32),
            pltpu.VMEM((M, M), BF16),
            pltpu.VMEM((M, M), BF16),
        ),
    )


def rho_of(codes, pick, faces, field, tables):
    flat = (tables.shape[1] // B, B)
    out = (shape(flat, F32), shape(flat, F32))
    ins = (codes, pick, *faces, field, tables)
    return call(rho_kernel, out, ins, 2, (pltpu.VMEM((NOV, NOV * B, B), F32),))


def gram_of(pick, potential, tables):
    return call(
        gram_kernel,
        shape((RMAX, B, B), BF16),
        (pick, potential, tables),
        1,
        (pltpu.VMEM(tables.shape, BF16), pltpu.VMEM((NOV, NOV * B, B), F32)),
    )


def returned_of(targets, slots, here, grams):
    tables = (targets, slots, here)
    whole = shape((N * N, B, B), BF16)
    early = call(early_kernel, whole, (*tables, *(grams[k] for k in EARLY)), 3)
    out = (shape((N, len(NEAR), B, B), BF16),) + (shape((len(FAR), B, B), BF16),) * N
    ins = (*tables, early, *(grams[k] for k in LATE))
    out = call(return_kernel, out, ins, 3, (pltpu.VMEM(whole.shape, BF16),))
    return out[0], out[1:]


def ring(step):
    size = lax.axis_size("gz")
    return [(i, (i + step) % size) for i in range(size)]


def both_ways(up, down):
    return (lax.ppermute(up, "gz", ring(1)), lax.ppermute(down, "gz", ring(-1)))


def across(x):
    return lax.all_to_all(x, "gy", split_axis=0, concat_axis=0, tiled=True)


def hand_over(far):
    size = lax.axis_size("gy")
    swapped = lax.ppermute(far[-1], "gy", [(i, i ^ 1) for i in range(size)])
    out = []
    for step, own in enumerate(far[:-1]):
        both = jnp.concatenate([own, swapped[step * len(FAR) : (step + 1) * len(FAR)]])
        if step:
            pairs = [(i, (i + 2 * step) % size) for i in range(size)]
            both = lax.ppermute(both, "gy", pairs)
        out.append(both)
    return out


def hand_back(far):
    size = lax.axis_size("gy")
    out = [far[0]]
    for step in range(1, size):
        out.append(lax.ppermute(far[step], "gy", [(i, (i + step) % size) for i in range(size)]))
    return out


def fetched(table, here, ham_blocks):
    up1, down1 = both_ways(ham_blocks, ham_blocks)
    up2, down2 = both_ways(up1, down1)
    up3, down3 = both_ways(up2, down2)
    up4 = lax.ppermute(up3, "gz", ring(1))
    own = call(hold_kernel, shape(ham_blocks.shape, BF16), (ham_blocks,), 0)
    ins = (table, here, own, up1, down1, up2, down2)
    near = call(near_kernel, shape((N, len(NEAR), B, B), BF16), ins, 2)
    near = across(near)
    ins = (table, here, up3, down3, up4)
    far = call(far_kernel, FAR_OUT, ins, 2)
    far = hand_over(far)
    return near, far


def brought_back(table, here, near, far):
    def sums(kernel, chosen, parts):
        out = (shape((HELD, B, B), F32),) * len(chosen)
        return call(functools.partial(kernel, chosen), out, (table, here, *parts), 2)

    far = hand_back(far)
    near = across(near)
    (up,) = sums(far_sums_kernel, (2,), far)
    up = lax.ppermute(up.astype(BF16), "gz", ring(1))
    down3, up3 = sums(far_sums_kernel, (0, 1), far)
    down = lax.ppermute(down3.astype(BF16), "gz", ring(-1))
    up = lax.ppermute((up3 + up.astype(F32)).astype(BF16), "gz", ring(1))
    down2, up2 = sums(near_sums_kernel, (3, 4), (near,))
    down = lax.ppermute((down2 + down.astype(F32)).astype(BF16), "gz", ring(-1))
    up = lax.ppermute((up2 + up.astype(F32)).astype(BF16), "gz", ring(1))
    own, down1, up1 = sums(near_sums_kernel, (0, 1, 2), (near,))
    down = lax.ppermute((down1 + down.astype(F32)).astype(BF16), "gz", ring(-1))
    up = lax.ppermute((up1 + up.astype(F32)).astype(BF16), "gz", ring(1))
    return own + down.astype(F32) + up.astype(F32)


def shards(
    ham_blocks, onsite, entry_slot, send_table, reads, gram_targets, table_pick, phi, potential_in
):
    slot_ids = entry_slot[0]
    pick = table_pick.reshape(-1)
    tables = phi.reshape(NOV * B, -1)
    tables = call(hold_kernel, shape(tables.shape, BF16), (tables,), 0)
    field = potential_in.reshape(-1, B)
    here = jnp.stack([lax.axis_index("gz"), lax.axis_index("gy")]).astype(jnp.int32)
    sent = pl.pallas_call(
        turn_kernel, out_shape=shape((N, 1, N), jnp.int32), in_specs=[SMEM], out_specs=SMEM
    )(send_table.reshape(-1))
    table = lax.all_to_all(sent, "gz", split_axis=0, concat_axis=0, tiled=True)
    near, far = fetched(table, here, ham_blocks)
    density = density_of(slot_ids, here, near, far, onsite, field)
    faces = face_exchange(density)
    source, first = rho_of(reads[0], pick, faces, field, tables)
    dims = potential_in.shape
    potential = jacobi_step(extended(first.reshape(dims)), source.reshape(dims))
    grams = gram_of(pick, potential.reshape(-1, B), tables)
    near, far = returned_of(gram_targets.reshape(-1), slot_ids, here, face_exchange(grams))
    return (potential, brought_back(table, here, near, far))


def solution(mesh):
    whole = ("gx", "gy", "gz")
    placed = (
        P(whole, None, None),
        P(whole, None),
        P(whole, None),
        P(whole, None, None),
        P(whole, None),
        P(whole, None, None),
        P(whole, None, None),
        P(whole, None, None, None),
        P("gx", "gy", "gz"),
    )
    return jax.shard_map(
        shards,
        mesh=mesh,
        in_specs=placed,
        out_specs=(P("gx", "gy", "gz"), P(whole, None, None)),
        check_vma=False,
    )
```
